128 devices in a mesh: row: 8 (over z, core), col: 16 (over y, x).
Axes of the slice: x: 4, y: 4, z: 4, core: 2. Of those that a mesh axis runs over, the one named last changes fastest.
Arguments:
- tokens: bfloat16 [16384, 4096], P(('row', 'col')), may hold values from -6 to 6
- router_logits: float32 [16384, 128], P(('row', 'col')), may hold values from -15 to 320
- expert_ids: int32 [16384, 8], P(('row', 'col')), may hold values from 0 to 127, all different within a row; in each aligned block of 128 rows (0 to 127, 128 to 255, ...) at most 12 rows name the same one
- w_gate: bfloat16 [128, 4096, 768], P(('row', 'col')), may hold values from -0.09375 to 0.09375
- w_up: bfloat16 [128, 4096, 768], P(('row', 'col')), may hold values from -0.09375 to 0.09375
- w_down: bfloat16 [128, 768, 4096], P(('row', 'col')), may hold values from -0.21875 to 0.21875
Outputs:
- mixed: bfloat16 [16384, 4096], P(('row', 'col'))
- balance_loss: float32 [], replicated
The draws below stay inside these ranges and needn't reach their ends.
Inputs may be any that keep to these rules, and one draw needn't show every extreme that they name: `expert_ids`: each row names 8 different experts. In the 128 rows of one device no expert is named by more than 12 rows, a bound that some block reaches.
All inputs are finite; a program needn't handle non-finite values.
Results may differ from the reference program's by a relative error of at most 0.0015.
The reference program's roundings to bfloat16 on the way count: a program that leaves them out, or rounds other values in their place, can miss the bound.
Values may be sent and summed in bfloat16 or wider, within the bound.
No kernel may reach another device: no remote copies, remote signals or barrier semaphores. Data moves between devices by JAX's collectives and lax.ppermute only.
A program may use at most 128 MiB of HBM per device.

```python
import math
import jax
import jax.numpy as jnp
import numpy as np
from jax import lax

D = 4096
FF = 768
TOPK = 8
TOK_DEV = 128
EXPERTS = 128
TOKENS = 16384
CAP = 12
N_ROW = 8
N_COL = 16


def draw_router_logits(key, part):
    base_key = jax.random.fold_in(key, 0)
    expert_key = jax.random.fold_in(key, 2)
    noise = 3.0 * jax.random.normal(base_key, (TOKENS, EXPERTS), jnp.float32)
    row_ids = jnp.arange(TOKENS)
    blocks = TOKENS // TOK_DEV
    block_of = (row_ids // TOK_DEV).astype(jnp.float32)
    rising = block_of / max(blocks - 1, 1)
    amplitude = 1.0 + 3.0 * rising
    expert_bias = 1.5 * jax.random.normal(expert_key, (EXPERTS,), jnp.float32)
    columns = jnp.arange(EXPERTS)
    phase = columns.astype(jnp.float32)[None, :] / EXPERTS - block_of[:, None] / blocks
    bias = amplitude[:, None] * jnp.cos(2.0 * jnp.pi * phase) + expert_bias[None, :]
    logits = jnp.clip(noise + bias, -15.0, 15.0)
    return logits


def levels(rng, dims, cuts, smallest, largest):
    def one(dim, shards_of):
        heights = jax.random.uniform(jax.random.fold_in(jax.random.fold_in(rng, 6), dim), (shards_of,), jnp.float32, smallest / len(cuts), largest / len(cuts))
        return jnp.repeat(jnp.exp(heights), dims[dim] // shards_of).reshape((-1,) + (1,) * (len(dims) - dim - 1))

    level = one(*cuts[0])
    for cut in cuts[1:]:
        level = level * one(*cut)
    return level


def assign_block(rng, own, number, rows, number_of, top, reach, lean):
    sequence = jax.random.permutation(rng, number_of)
    heavy_load, ordinary = load_shares(number_of, rows * top, reach, lean, True), load_shares(number_of, rows * top, reach, lean, False)
    places = jnp.arange(number_of)

    def named(tallies, offset_by):
        used = int((tallies > 0).sum())
        fixed = max(1, used // 4)
        shifted = fixed + (places - fixed + offset_by * (used - fixed)) % max(1, number_of - fixed)
        return jnp.zeros((number_of,), jnp.int32).at[sequence[jnp.where(places < fixed, places, shifted)]].set(jnp.asarray(tallies, jnp.int32))

    tallies = jnp.where(number % 4 == 0, named(heavy_load, number // 4), named(ordinary, number - number // 4 - 1))
    mixed = jax.random.permutation(jax.random.fold_in(own, 3), number_of)
    giver, taker = mixed[0:number_of // 2 * 2:2], mixed[1:number_of // 2 * 2:2]
    margin = jnp.minimum(tallies[giver] - 1, reach - tallies[taker]) // 2
    margin = jnp.where((giver == sequence[0]) | (taker == sequence[0]) | (tallies[taker] == 0), 0, jnp.maximum(margin, 0))
    shifted = jax.random.randint(jax.random.fold_in(own, 4), (number_of // 2,), 0, 1 << 20) % (margin + 1)
    tallies = tallies.at[giver].add(-shifted).at[taker].add(shifted)
    members = jnp.searchsorted(jnp.cumsum(tallies), jnp.arange(rows * top), side="right").astype(jnp.int32)
    table = members.reshape(top, rows).T
    table = table[jax.random.permutation(jax.random.fold_in(own, 1), rows)]
    offset_by = jax.random.randint(jax.random.fold_in(own, 2), (rows, 1), 0, top)
    return jnp.take_along_axis(table, (jnp.arange(top)[None, :] + offset_by) % top, axis=1)


def load_shares(number_of, total, most, lean, full):
    loads = [(1 << 20) // math.isqrt(grade ** lean) + 1 for grade in range(1, number_of + 1)]
    largest = most if full else min(most, max(-(-total // number_of), total * loads[0] // sum(loads)))
    least = 1 if total - largest >= number_of - 1 else 0
    holding, surplus = [largest] + [least] * (number_of - 1), total - largest - least * (number_of - 1)
    while surplus > 0:
        free = [i for i in range(1, number_of) if holding[i] < largest] or [i for i in range(1, number_of) if holding[i] < most]
        whole, budget = sum([loads[i] for i in free]), surplus
        for i in free:
            extra = min(most - holding[i], max(1, budget * loads[i] // whole), surplus)
            holding[i] = holding[i] + extra
            surplus = surplus - extra
    return np.array(holding)


def normal_values(key, extent, width, most, shards=(), held_as=jnp.bfloat16):
    gain = levels(key, extent, shards, -0.22, 0.18) if shards else 1.0
    drawn = jax.random.normal(key, extent, jnp.float32) * width * gain
    return jnp.minimum(jnp.maximum(drawn, -most), most).astype(held_as)


def setup_inputs(seed: int = 0) -> dict:
    arg_keys = jax.random.split(jax.random.key(seed), 7)
    tokens = normal_values(arg_keys[0], (TOKENS, D), 1.0, 6.0, ((0, 128),))
    router_logits = draw_router_logits(jax.random.fold_in(arg_keys[6], 71), 0)
    expert_ids_keys = jax.random.split(jax.random.fold_in(arg_keys[2], 1), TOKENS // TOK_DEV)
    expert_ids_turns = jax.random.permutation(jax.random.fold_in(arg_keys[2], 3), TOKENS // TOK_DEV)
    expert_ids = jax.vmap(lambda own, number: assign_block(jax.random.fold_in(arg_keys[2], 2), own, number, TOK_DEV, EXPERTS, TOPK, CAP, 2))(expert_ids_keys, expert_ids_turns).reshape((TOKENS, TOPK))
    w_gate = normal_values(arg_keys[3], (EXPERTS, D, FF), D ** -0.5, 0.09375, ((0, 128),))
    w_up = normal_values(arg_keys[4], (EXPERTS, D, FF), D ** -0.5, 0.09375, ((0, 128),))
    w_down = normal_values(arg_keys[5], (EXPERTS, FF, D), FF ** -0.5, 0.21875, ((0, 128),))
    return {"tokens": tokens, "router_logits": router_logits, "expert_ids": expert_ids, "w_gate": w_gate, "w_up": w_up, "w_down": w_down}


def slot_table(expert_ids, experts, capacity):
    flattened = expert_ids.reshape(-1)
    onehot = (flattened[:, None] == jnp.arange(experts, dtype=jnp.int32)[None, :]).astype(jnp.int32)
    earlier = jnp.cumsum(onehot, axis=0) - onehot
    slot_of = jnp.sum(earlier * onehot, axis=1)
    position = flattened * capacity + slot_of
    return onehot, position.astype(jnp.int32)


def reference(tokens, router_logits, expert_ids, w_gate, w_up, w_down):
    blocks = N_ROW * N_COL
    assigned = TOK_DEV * TOPK
    probs = jax.nn.softmax(router_logits.astype(jnp.float32), axis=1)
    chosen = jnp.take_along_axis(probs, expert_ids, axis=1)
    weights = chosen / jnp.sum(chosen, axis=1, keepdims=True)
    grouped_ids = expert_ids.reshape(blocks, TOK_DEV, TOPK)
    onehot, position = jax.vmap(slot_table, in_axes=(0, None, None))(grouped_ids, EXPERTS, CAP)
    block_ids = jnp.arange(blocks, dtype=jnp.int32)
    source = block_ids[:, None] * TOK_DEV + jnp.arange(assigned, dtype=jnp.int32)[None, :] // TOPK
    owner = jnp.full((blocks, EXPERTS * CAP), -1, jnp.int32).at[block_ids[:, None], position].set(source)
    weight_table = jnp.zeros((blocks, EXPERTS * CAP), jnp.float32).at[block_ids[:, None], position].set(weights.reshape(blocks, assigned))
    owner = owner.reshape(blocks, EXPERTS, CAP).transpose(1, 0, 2).reshape(EXPERTS, blocks * CAP)
    weight_table = weight_table.reshape(blocks, EXPERTS, CAP).transpose(1, 0, 2).reshape(EXPERTS, blocks * CAP)

    def one_expert(total, inputs):
        owner_e, weight_e, gate_e, up_e, down_e = inputs
        present = owner_e >= 0
        safe = jnp.maximum(owner_e, 0).astype(jnp.int32)
        slot_rows = jnp.where(present[:, None], tokens[safe], jnp.zeros((), jnp.bfloat16))
        gate_act = jnp.dot(slot_rows, gate_e, preferred_element_type=jnp.float32)
        up_act = jnp.dot(slot_rows, up_e, preferred_element_type=jnp.float32)
        hidden = (jax.nn.silu(gate_act) * up_act).astype(jnp.bfloat16)
        result = jnp.dot(hidden, down_e, preferred_element_type=jnp.float32).astype(jnp.bfloat16)
        total = total.at[safe].add(weight_e[:, None] * result.astype(jnp.float32))
        return total, None

    start = jnp.zeros((TOKENS, D), jnp.float32)
    total, unused = lax.scan(one_expert, start, (owner, weight_table, w_gate, w_up, w_down))
    mixed = total.astype(jnp.bfloat16)
    counts = jnp.sum(onehot, axis=(0, 1)).astype(jnp.float32)
    prob_total = jnp.sum(probs, axis=0)
    balance_loss = EXPERTS * jnp.sum((counts / (TOKENS * TOPK)) * (prob_total / TOKENS))
    return mixed, balance_loss
```

```python
import functools

import jax
import jax.numpy as jnp
from jax import lax
from jax.experimental import pallas as pl
from jax.experimental.pallas import tpu as pltpu
from jax.sharding import Mesh
from jax.sharding import PartitionSpec as P

ROW_COL = ("row_0", "row_1", "col_0", "col_1")
BF = jnp.bfloat16
F32 = jnp.float32
NONE = 255.0
FULL = 8
HALF = 4
LANES = 128


def iota(shape, dim):
    return lax.broadcasted_iota(jnp.int32, shape, dim)


def dot(a, b):
    return lax.dot_general(a, b, (((1,), (0,)), ((), ())), preferred_element_type=F32)


def chosen_by_expert(ids_ref, experts):
    top_k, tok = ids_ref.shape
    rows = iota((experts, tok), 0)
    hit = jnp.zeros((experts, tok), F32)
    for k in range(top_k):
        hit = hit + jnp.where(rows == ids_ref[k : k + 1, :], 1.0, 0.0)
    return hit


def slots_by_expert(ids_ref, experts):
    tok = ids_ref.shape[1]
    hit = chosen_by_expert(ids_ref, experts)
    before = jnp.where(iota((tok, tok), 0) < iota((tok, tok), 1), 1.0, 0.0).astype(BF)
    earlier = dot(hit.astype(BF), before)
    return hit, jnp.where(hit > 0.0, earlier, NONE)


def probabilities(logits):
    shifted = jnp.exp(logits - jnp.max(logits, axis=1, keepdims=True))
    return shifted / jnp.sum(shifted, axis=1, keepdims=True)


def three_terms(x):
    high = x.astype(BF)
    rest = x - high.astype(F32)
    mid = rest.astype(BF)
    low = (rest - mid.astype(F32)).astype(BF)
    return high, mid, low


def spread_rows(slots, step, rows, experts):
    pick = iota((rows, experts), 0) // 8 + step * (rows // 8) == iota((rows, experts), 1)
    return dot(jnp.where(pick, 1.0, 0.0).astype(BF), slots)


def send_full_kernel(ids_ref, tok_ref, out_ref, slots_ref):
    step = pl.program_id(0)
    rows = out_ref.shape[0]
    experts = slots_ref.shape[0]

    @pl.when(step == 0)
    def _():
        slots_ref[...] = slots_by_expert(ids_ref, experts)[1].astype(BF)

    wide = spread_rows(slots_ref[...], step, rows, experts)
    want = (iota(wide.shape, 0) % 8).astype(F32)
    select = jnp.where(wide == want, 1.0, 0.0).astype(BF)
    out_ref[...] = dot(select, tok_ref[...]).astype(BF)


def send_half_kernel(ids_ref, logits_ref, tok_ref, out_ref, slots_ref, stat_ref):
    step = pl.program_id(0)
    rows = out_ref.shape[0]
    experts = slots_ref.shape[0]
    half = tok_ref.shape[1] // 2

    @pl.when(step == 0)
    def _():
        hit, slots = slots_by_expert(ids_ref, experts)
        slots_ref[...] = slots.astype(BF)
        counts = jnp.sum(hit.T, axis=0, keepdims=True)
        sums = jnp.sum(probabilities(logits_ref[...]), axis=0, keepdims=True)
        high, mid, low = three_terms(sums)
        line = iota((8, experts), 0)
        tile = jnp.where(line == 0, counts, 0.0)
        for number, term in ((1, high), (2, mid), (3, low)):
            tile = jnp.where(line == number, term.astype(F32), tile)
        stat_ref[...] = tile

    wide = spread_rows(slots_ref[...], step, rows, experts)
    line = iota(wide.shape, 0) % 8
    match = wide == (FULL + line % HALF).astype(F32)
    first = jnp.where(match & (line < HALF), 1.0, 0.0).astype(BF)
    second = jnp.where(match & (line >= HALF), 1.0, 0.0).astype(BF)
    body = dot(first, tok_ref[:, :half]) + dot(second, tok_ref[:, half:])
    out_ref[:, :half] = body.astype(BF)
    stats = jnp.broadcast_to(stat_ref[...][None], (rows // 8, 8, experts)).reshape(rows, experts)
    out_ref[:, half:] = stats.astype(BF)


def silu_times(gate, up):
    return gate * (1.0 / (1.0 + jnp.exp(-gate))) * up


def ffn_full_kernel(x_ref, gate_ref, up_ref, down_ref, out_ref):
    x = x_ref[...]
    hidden = silu_times(dot(x, gate_ref[...]), dot(x, up_ref[...])).astype(BF)
    out_ref[...] = dot(hidden, down_ref[...]).astype(BF)


def join_halves(x, weight_ref):
    half = x.shape[1]
    line = iota((x.shape[0], weight_ref.shape[1]), 0) % 8
    own = jnp.where(line < HALF, dot(x, weight_ref[:half]), dot(x, weight_ref[half:]))
    own = own.reshape(x.shape[0] // 8, 8, weight_ref.shape[1])
    return (own + pltpu.roll(own, HALF, 1)).reshape(x.shape[0], weight_ref.shape[1])


def ffn_half_kernel(x_ref, gate_ref, up_ref, down_ref, out_ref):
    x = x_ref[...]
    half = x.shape[1]
    hidden = silu_times(join_halves(x, gate_ref), join_halves(x, up_ref)).astype(BF)
    line = iota((x.shape[0], half), 0) % 8
    low, high = dot(hidden, down_ref[:, :half]), dot(hidden, down_ref[:, half:])
    out_ref[...] = jnp.where(line < HALF, low, high).astype(BF)


def weights_kernel(ids_ref, logits_ref, full_ref, half_ref):
    tok, experts = logits_ref.shape
    hit, slots = slots_by_expert(ids_ref, experts)
    hit = hit.T
    slots = slots.T
    chosen = jnp.where(hit > 0.0, probabilities(logits_ref[...]), 0.0)
    weights = chosen / jnp.sum(chosen, axis=1, keepdims=True)
    columns = experts * 8
    spread = jnp.where(iota((experts, columns), 1) // 8 == iota((experts, columns), 0), 1.0, 0.0).astype(BF)
    wide = dot(slots.astype(BF), spread)
    line = iota(wide.shape, 1) % 8
    in_full = wide == line.astype(F32)
    in_half = wide == (FULL + line % HALF).astype(F32)
    for number, term in enumerate(three_terms(weights)):
        value = dot(term, spread)
        rows = slice(number * tok, (number + 1) * tok)
        full_ref[rows, :] = jnp.where(in_full, value, 0.0).astype(BF)
        half_ref[0, rows, :] = jnp.where(in_half & (line < HALF), value, 0.0).astype(BF)
        half_ref[1, rows, :] = jnp.where(in_half & (line >= HALF), value, 0.0).astype(BF)


def add_terms(product):
    tok = product.shape[0] // 3
    return product[:tok] + (product[tok : 2 * tok] + product[2 * tok :])


def sum_full_kernel(weights_ref, x_ref, out_ref):
    out_ref[...] = add_terms(dot(weights_ref[...], x_ref[...]))


def sum_half_kernel(weights_ref, x_ref, sofar_ref, out_ref):
    own = add_terms(dot(weights_ref[pl.program_id(1)], x_ref[...]))
    out_ref[...] = (sofar_ref[...] + own).astype(BF)


def whole(shape):
    zeros = (0,) * len(shape)
    return pl.BlockSpec(shape, lambda *_: zeros, pipeline_mode=pl.Buffered(1))


def call(kernel, grid, out_shape, in_specs, out_specs, flops, moved, scratch=()):
    return pl.pallas_call(
        kernel,
        grid=grid,
        out_shape=out_shape,
        in_specs=in_specs,
        out_specs=out_specs,
        scratch_shapes=scratch,
        cost_estimate=pl.CostEstimate(flops=flops, bytes_accessed=moved, transcendentals=0),
        compiler_params=pltpu.CompilerParams(
            dimension_semantics=("arbitrary",) * len(grid), vmem_limit_bytes=56 * 2**20
        ),
    )


def local(tokens, router_logits, expert_ids, w_gate, w_up, w_down):
    tok, top_k = expert_ids.shape
    width = tokens.shape[1]
    experts = router_logits.shape[1]
    ff = w_gate.shape[2]
    devices = lax.axis_size(ROW_COL)
    half = width // 2
    lines = experts * 8
    block = 256
    steps = lines // block
    ids = expert_ids.T
    gate, up, down = w_gate[0], w_up[0], w_down[0]
    rows = lambda lanes: pl.BlockSpec((block, lanes), lambda i: (i, 0))
    shape = jax.ShapeDtypeStruct
    slots_scratch = pltpu.VMEM((experts, tok), BF)

    def exchange(x):
        lanes = x.shape[1]
        moved = lax.all_to_all(
            x.reshape(experts, 8, lanes), ROW_COL, split_axis=0, concat_axis=0, tiled=True
        )
        return moved.reshape(lines, lanes)

    send_full = call(
        send_full_kernel,
        (steps,),
        shape((lines, width), BF),
        [whole(ids.shape), whole(tokens.shape)],
        rows(width),
        2 * lines * tok * width,
        2 * lines * width,
        (slots_scratch,),
    )(ids, tokens)
    send_half = call(
        send_half_kernel,
        (steps,),
        shape((lines, half + LANES), BF),
        [whole(ids.shape), whole(router_logits.shape), whole(tokens.shape)],
        rows(half + LANES),
        4 * lines * tok * half,
        2 * lines * half,
        (slots_scratch, pltpu.VMEM((8, experts), F32)),
    )(ids, router_logits, tokens)
    weights_full, weights_half = call(
        weights_kernel,
        (1,),
        (shape((3 * tok, lines), BF), shape((2, 3 * tok, lines), BF)),
        [whole(ids.shape), whole(router_logits.shape)],
        (whole((3 * tok, lines)), whole((2, 3 * tok, lines))),
        8 * tok * experts * lines,
        18 * tok * lines,
    )(ids, router_logits)

    weight_specs = [whole(gate.shape), whole(up.shape), whole(down.shape)]
    got_full = exchange(send_full)
    made_full = call(
        ffn_full_kernel,
        (steps,),
        shape((lines, width), BF),
        [rows(width)] + weight_specs,
        rows(width),
        6 * lines * width * ff,
        4 * lines * width + 6 * width * ff,
    )(got_full, gate, up, down)
    got_half = exchange(send_half)
    made_half = call(
        ffn_half_kernel,
        (steps,),
        shape((lines, half), BF),
        [rows(half)] + weight_specs,
        rows(half),
        6 * lines * width * ff,
        2 * lines * width + 6 * width * ff,
    )(got_half, gate, up, down)

    back_full = exchange(made_full)
    lanes = width // 4
    part = call(
        sum_full_kernel,
        (4,),
        shape((tok, width), F32),
        [whole(weights_full.shape), pl.BlockSpec((lines, lanes), lambda i: (0, i))],
        pl.BlockSpec((tok, lanes), lambda i: (0, i)),
        6 * tok * lines * width,
        2 * lines * width,
    )(weights_full, back_full)
    back_half = exchange(made_half)
    lanes = half // 4
    at = pl.BlockSpec((tok, lanes), lambda i, h: (0, h * 4 + i))
    mixed = call(
        sum_half_kernel,
        (4, 2),
        shape((tok, width), BF),
        [whole(weights_half.shape), pl.BlockSpec((lines, lanes), lambda i, h: (0, i)), at],
        at,
        6 * tok * lines * width,
        2 * lines * half,
    )(weights_half, back_half, part)

    stats = got_half.reshape(devices, 8, half + LANES)[:, :4, half : half + experts]
    stats = jnp.sum(stats.astype(F32), axis=0)
    total_counts = stats[0]
    total_probs = stats[1] + (stats[2] + stats[3])
    tokens_all = tok * devices
    balance_loss = experts * jnp.sum(
        total_counts / (tokens_all * top_k) * (total_probs / tokens_all)
    )
    return mixed, balance_loss


def solution(mesh):
    torus = Mesh(mesh.devices.reshape(4, 2, 4, 4), ROW_COL)
    rows = P(ROW_COL, None)
    expert = P(ROW_COL, None, None)
    return jax.shard_map(
        local,
        mesh=torus,
        in_specs=(rows, rows, rows, expert, expert, expert),
        out_specs=(rows, P()),
        check_vma=False,
    )
```

```python
import functools

import jax
import jax.numpy as jnp
from jax import lax
from jax.experimental import pallas as pl
from jax.experimental.pallas import tpu as pltpu
from jax.sharding import Mesh
from jax.sharding import PartitionSpec as P

ROW_COL = ("row_0", "row_1", "col_0", "col_1")
BF = jnp.bfloat16
F32 = jnp.float32
NONE = 255.0
FULL = 8
HALF = 4


def iota(shape, dim):
    return lax.broadcasted_iota(jnp.int32, shape, dim)


def dot(a, b):
    return lax.dot_general(a, b, (((1,), (0,)), ((), ())), preferred_element_type=F32)


def chosen_by_expert(ids_ref, experts):
    top_k, tok = ids_ref.shape
    rows = iota((experts, tok), 0)
    hit = jnp.zeros((experts, tok), F32)
    for k in range(top_k):
        hit = hit + jnp.where(rows == ids_ref[k : k + 1, :], 1.0, 0.0)
    return hit


def slots_by_expert(ids_ref, experts):
    tok = ids_ref.shape[1]
    hit = chosen_by_expert(ids_ref, experts)
    before = jnp.where(iota((tok, tok), 0) < iota((tok, tok), 1), 1.0, 0.0).astype(BF)
    earlier = dot(hit.astype(BF), before)
    return hit, jnp.where(hit > 0.0, earlier, NONE)


def probabilities(logits):
    shifted = jnp.exp(logits - jnp.max(logits, axis=1, keepdims=True))
    return shifted / jnp.sum(shifted, axis=1, keepdims=True)


def three_terms(x):
    high = x.astype(BF)
    rest = x - high.astype(F32)
    mid = rest.astype(BF)
    low = (rest - mid.astype(F32)).astype(BF)
    return high, mid, low


def spread_rows(slots, step, rows, experts):
    pick = iota((rows, experts), 0) // 8 + step * (rows // 8) == iota((rows, experts), 1)
    return dot(jnp.where(pick, 1.0, 0.0).astype(BF), slots)


def send_kernel(ids_ref, logits_ref, hbm_ref, out_ref, tok_ref, arrived):
    tok, width = tok_ref.shape
    experts = logits_ref.shape[1]
    half = width // 2
    fetch = pltpu.make_async_copy(hbm_ref, tok_ref, arrived)
    fetch.start()
    hit, slots = slots_by_expert(ids_ref, experts)
    slots = slots.astype(BF)
    counts = jnp.sum(hit.T, axis=0, keepdims=True)
    sums = jnp.sum(probabilities(logits_ref[...]), axis=0, keepdims=True)
    line = iota((8, experts), 0)
    tile = jnp.where(line == 0, counts, 0.0)
    for number, term in enumerate(three_terms(sums)):
        tile = jnp.where(line == number + 1, term.astype(F32), tile)
    rows = 256
    stats = jnp.broadcast_to(tile[None], (rows // 8, 8, experts)).reshape(rows, experts).astype(BF)
    fetch.wait()
    for step in range(experts * 8 // rows):
        at = slice(step * rows, (step + 1) * rows)
        wide = spread_rows(slots, step, rows, experts)
        line = iota(wide.shape, 0) % 8
        full = jnp.where(wide == line.astype(F32), 1.0, 0.0).astype(BF)
        out_ref[at, :width] = dot(full, tok_ref[...]).astype(BF)
        match = wide == (FULL + line % HALF).astype(F32)
        first = jnp.where(match & (line < HALF), 1.0, 0.0).astype(BF)
        second = jnp.where(match & (line >= HALF), 1.0, 0.0).astype(BF)
        body = dot(first, tok_ref[:, :half]) + dot(second, tok_ref[:, half:])
        out_ref[at, width : width + half] = body.astype(BF)
        out_ref[at, width + half :] = stats


def silu_times(gate, up):
    return gate * (1.0 / (1.0 + jnp.exp(-gate))) * up


def ffn_full_kernel(x_ref, gate_ref, up_ref, down_ref, out_ref):
    x = x_ref[...]
    hidden = silu_times(dot(x, gate_ref[...]), dot(x, up_ref[...])).astype(BF)
    out_ref[...] = dot(hidden, down_ref[...]).astype(BF)


def swap_halves(first, second):
    low = iota(first.shape, 1) < HALF
    return (
        jnp.where(low, first, pltpu.roll(second, HALF, 1)),
        jnp.where(low, pltpu.roll(first, HALF, 1), second),
    )


def ffn_half_kernel(x_ref, gate_ref, up_ref, down_ref, out_ref):
    lines, half = x_ref.shape
    pairs = x_ref[...].astype(F32).reshape(lines // 16, 2, 8, half)
    first, second = swap_halves(pairs[:, 0], pairs[:, 1])
    first = first.reshape(lines // 2, half).astype(BF)
    second = second.reshape(lines // 2, half).astype(BF)
    gate = dot(first, gate_ref[:half]) + dot(second, gate_ref[half:])
    up = dot(first, up_ref[:half]) + dot(second, up_ref[half:])
    hidden = silu_times(gate, up).astype(BF)
    tiles = (lines // 16, 8, half)
    first = dot(hidden, down_ref[:, :half]).reshape(tiles)
    second = dot(hidden, down_ref[:, half:]).reshape(tiles)
    first, second = swap_halves(first, second)
    out_ref[...] = jnp.stack([first, second], axis=1).reshape(lines, half).astype(BF)


def weights_kernel(ids_ref, logits_ref, full_ref, half_ref):
    tok, experts = logits_ref.shape
    hit, slots = slots_by_expert(ids_ref, experts)
    hit = hit.T
    slots = slots.T
    chosen = jnp.where(hit > 0.0, probabilities(logits_ref[...]), 0.0)
    weights = chosen / jnp.sum(chosen, axis=1, keepdims=True)
    columns = experts * 8
    spread = jnp.where(iota((experts, columns), 1) // 8 == iota((experts, columns), 0), 1.0, 0.0).astype(BF)
    wide = dot(slots.astype(BF), spread)
    line = iota(wide.shape, 1) % 8
    in_full = wide == line.astype(F32)
    in_half = wide == (FULL + line % HALF).astype(F32)
    for number, term in enumerate(three_terms(weights)[:2]):
        value = dot(term, spread)
        rows = slice(number * tok, (number + 1) * tok)
        full_ref[rows, :] = jnp.where(in_full, value, 0.0).astype(BF)
        half_ref[0, rows, :] = jnp.where(in_half & (line < HALF), value, 0.0).astype(BF)
        half_ref[1, rows, :] = jnp.where(in_half & (line >= HALF), value, 0.0).astype(BF)


def add_terms(product):
    tok = product.shape[0] // 2
    return product[:tok] + product[tok:]


def sum_half_kernel(weights_ref, x_ref, out_ref):
    for side in range(2):
        out_ref[side] = add_terms(dot(weights_ref[side], x_ref[...]))


def sum_full_kernel(weights_ref, x_ref, sofar_ref, out_ref):
    out_ref[...] = (sofar_ref[0] + add_terms(dot(weights_ref[...], x_ref[...]))).astype(BF)


def whole(shape):
    zeros = (0,) * len(shape)
    return pl.BlockSpec(shape, lambda *_: zeros, pipeline_mode=pl.Buffered(1))


def call(kernel, grid, out_shape, in_specs, out_specs, flops, moved, limit=20, scratch=()):
    return pl.pallas_call(
        kernel,
        grid=grid,
        out_shape=out_shape,
        in_specs=in_specs,
        out_specs=out_specs,
        scratch_shapes=scratch,
        name=kernel.__name__,
        cost_estimate=pl.CostEstimate(flops=flops, bytes_accessed=moved, transcendentals=0),
        compiler_params=pltpu.CompilerParams(
            dimension_semantics=("arbitrary",) * len(grid), vmem_limit_bytes=limit * 2**20
        ),
    )


def local(tokens, router_logits, expert_ids, w_gate, w_up, w_down):
    tok, top_k = expert_ids.shape
    width = tokens.shape[1]
    experts = router_logits.shape[1]
    ff = w_gate.shape[2]
    devices = lax.axis_size(ROW_COL)
    half = width // 2
    lines = experts * 8
    ids = expert_ids.T
    in_vmem = lambda x: pltpu.with_memory_space_constraint(x, pltpu.VMEM)
    in_hbm = lambda x: pltpu.with_memory_space_constraint(x, pltpu.HBM)
    resident = pl.BlockSpec(memory_space=pltpu.VMEM)
    gate, up, down = in_vmem(w_gate[0]), in_vmem(w_up[0]), in_vmem(w_down[0])
    shape = jax.ShapeDtypeStruct

    def exchange(x):
        lanes = x.shape[1]
        moved = lax.all_to_all(
            x.reshape(experts, 8, lanes), ROW_COL, split_axis=0, concat_axis=0, tiled=True
        )
        return moved.reshape(lines, lanes)

    sent = width + half + experts
    send = call(
        send_kernel,
        (),
        pltpu.VMEM((lines, sent), BF),
        [whole(ids.shape), whole(router_logits.shape), pl.BlockSpec(memory_space=pltpu.HBM)],
        resident,
        2 * lines * tok * (width + 2 * half),
        2 * lines * sent,
        scratch=(pltpu.VMEM(tokens.shape, BF), pltpu.SemaphoreType.DMA),
    )(in_hbm(ids), in_hbm(router_logits), in_hbm(tokens))
    got = exchange(send)
    made_half = call(
        ffn_half_kernel,
        (2,),
        pltpu.HBM((lines, half), BF),
        [pl.BlockSpec((lines // 2, half), lambda i: (i, 2))] + [resident] * 3,
        pl.BlockSpec((lines // 2, half), lambda i: (i, 0)),
        3 * lines * width * ff,
        2 * lines * width + 6 * width * ff,
        30,
    )(got, gate, up, down)
    back_half = exchange(made_half)
    made_full = call(
        ffn_full_kernel,
        (4,),
        pltpu.HBM((lines, width), BF),
        [pl.BlockSpec((lines // 4, width), lambda i: (i, 0))] + [resident] * 3,
        pl.BlockSpec((lines // 4, width), lambda i: (i, 0)),
        6 * lines * width * ff,
        4 * lines * width + 6 * width * ff,
        24,
    )(got, gate, up, down)
    back_full = exchange(made_full)

    weights_full, weights_half = call(
        weights_kernel,
        (),
        (shape((2 * tok, lines), BF), shape((2, 2 * tok, lines), BF)),
        [resident] * 2,
        (resident, resident),
        6 * tok * experts * lines,
        12 * tok * lines,
    )(ids, router_logits)
    lanes = half // 4
    part = call(
        sum_half_kernel,
        (4,),
        shape((2, tok, half), F32),
        [whole(weights_half.shape), pl.BlockSpec((lines, lanes), lambda i: (0, i))],
        pl.BlockSpec((2, tok, lanes), lambda i: (0, 0, i)),
        4 * tok * lines * width,
        2 * lines * half,
    )(weights_half, back_half)
    at = pl.BlockSpec((tok, lanes), lambda i: (0, i))
    mixed = call(
        sum_full_kernel,
        (8,),
        shape((tok, width), BF),
        [
            whole(weights_full.shape),
            pl.BlockSpec((lines, lanes), lambda i: (0, i)),
            pl.BlockSpec((1, tok, lanes), lambda i: (i // 4, 0, i % 4)),
        ],
        at,
        4 * tok * lines * width,
        2 * lines * width,
    )(weights_full, back_full, part)

    stats = got.reshape(devices, 8, sent)[:, :4, width + half :]
    stats = jnp.sum(stats.astype(F32), axis=0)
    total_counts = stats[0]
    total_probs = stats[1] + (stats[2] + stats[3])
    tokens_all = tok * devices
    balance_loss = experts * jnp.sum(
        total_counts / (tokens_all * top_k) * (total_probs / tokens_all)
    )
    return mixed, balance_loss


def solution(mesh):
    torus = Mesh(mesh.devices.reshape(4, 2, 4, 4), ROW_COL)
    rows = P(ROW_COL, None)
    expert = P(ROW_COL, None, None)
    return jax.shard_map(
        local,
        mesh=torus,
        in_specs=(rows, rows, rows, expert, expert, expert),
        out_specs=(rows, P()),
        check_vma=False,
    )
```

```python
import functools

import jax
import jax.numpy as jnp
from jax import lax
from jax.experimental import pallas as pl
from jax.experimental.pallas import tpu as pltpu
from jax.sharding import Mesh
from jax.sharding import PartitionSpec as P

ROW_COL = ("row_0", "row_1", "col_0", "col_1")
BF = jnp.bfloat16
F32 = jnp.float32
NONE = 255.0
FULL = 8
HALF = 4


def iota(shape, dim):
    return lax.broadcasted_iota(jnp.int32, shape, dim)


def dot(a, b):
    return lax.dot_general(a, b, (((1,), (0,)), ((), ())), preferred_element_type=F32)


def chosen_by_expert(ids_ref, experts):
    top_k, tok = ids_ref.shape
    rows = iota((experts, tok), 0)
    hit = jnp.zeros((experts, tok), F32)
    for k in range(top_k):
        hit = hit + jnp.where(rows == ids_ref[k : k + 1, :], 1.0, 0.0)
    return hit


def slots_by_expert(ids_ref, experts):
    tok = ids_ref.shape[1]
    hit = chosen_by_expert(ids_ref, experts)
    before = jnp.where(iota((tok, tok), 0) < iota((tok, tok), 1), 1.0, 0.0).astype(BF)
    earlier = dot(hit.astype(BF), before)
    return hit, jnp.where(hit > 0.0, earlier, NONE)


def probabilities(logits):
    shifted = jnp.exp(logits - jnp.max(logits, axis=1, keepdims=True))
    return shifted / jnp.sum(shifted, axis=1, keepdims=True)


def three_terms(x):
    high = x.astype(BF)
    rest = x - high.astype(F32)
    mid = rest.astype(BF)
    low = (rest - mid.astype(F32)).astype(BF)
    return high, mid, low


def spread_rows(slots, step, rows, experts):
    pick = iota((rows, experts), 0) // 8 + step * (rows // 8) == iota((rows, experts), 1)
    return dot(jnp.where(pick, 1.0, 0.0).astype(BF), slots)


def send_kernel(ids_ref, logits_ref, hbm_ref, out_ref, tok_ref, arrived):
    tok, width = tok_ref.shape
    experts = logits_ref.shape[1]
    half = width // 2
    fetch = pltpu.make_async_copy(hbm_ref, tok_ref, arrived)
    fetch.start()
    hit, slots = slots_by_expert(ids_ref, experts)
    slots = slots.astype(BF)
    counts = jnp.sum(hit.T, axis=0, keepdims=True)
    sums = jnp.sum(probabilities(logits_ref[...]), axis=0, keepdims=True)
    line = iota((8, experts), 0)
    tile = jnp.where(line == 0, counts, 0.0)
    for number, term in enumerate(three_terms(sums)):
        tile = jnp.where(line == number + 1, term.astype(F32), tile)
    rows = 256
    stats = jnp.broadcast_to(tile[None], (rows // 8, 8, experts)).reshape(rows, experts).astype(BF)
    fetch.wait()
    for step in range(experts * 8 // rows):
        at = slice(step * rows, (step + 1) * rows)
        wide = spread_rows(slots, step, rows, experts)
        line = iota(wide.shape, 0) % 8
        full = jnp.where(wide == line.astype(F32), 1.0, 0.0).astype(BF)
        out_ref[at, :width] = dot(full, tok_ref[...]).astype(BF)
        match = wide == (FULL + line % HALF).astype(F32)
        first = jnp.where(match & (line < HALF), 1.0, 0.0).astype(BF)
        second = jnp.where(match & (line >= HALF), 1.0, 0.0).astype(BF)
        body = dot(first, tok_ref[:, :half]) + dot(second, tok_ref[:, half:])
        out_ref[at, width : width + half] = body.astype(BF)
        out_ref[at, width + half :] = stats


def silu_times(gate, up):
    return gate * (1.0 / (1.0 + jnp.exp(-gate))) * up


def ffn_full_kernel(after_ref, x_ref, gate_ref, up_ref, down_ref, out_ref):
    x = x_ref[...]
    rows = x.shape[0]
    at = pl.ds(pl.multiple_of(pl.program_id(0) * rows, rows), rows)
    hidden = silu_times(dot(x, gate_ref[...]), dot(x, up_ref[...])).astype(BF)
    out_ref[at, :] = dot(hidden, down_ref[...]).astype(BF)


def swap_halves(first, second):
    low = iota(first.shape, 1) < HALF
    return (
        jnp.where(low, first, pltpu.roll(second, HALF, 1)),
        jnp.where(low, pltpu.roll(first, HALF, 1), second),
    )


def ffn_half_kernel(x_ref, gate_ref, up_ref, down_ref, out_ref):
    lines, half = x_ref.shape
    pairs = x_ref[...].astype(F32).reshape(lines // 16, 2, 8, half)
    first, second = swap_halves(pairs[:, 0], pairs[:, 1])
    first = first.reshape(lines // 2, half).astype(BF)
    second = second.reshape(lines // 2, half).astype(BF)
    gate = dot(first, gate_ref[:half]) + dot(second, gate_ref[half:])
    up = dot(first, up_ref[:half]) + dot(second, up_ref[half:])
    hidden = silu_times(gate, up).astype(BF)
    tiles = (lines // 16, 8, half)
    first = dot(hidden, down_ref[:, :half]).reshape(tiles)
    second = dot(hidden, down_ref[:, half:]).reshape(tiles)
    first, second = swap_halves(first, second)
    out_ref[...] = jnp.stack([first, second], axis=1).reshape(lines, half).astype(BF)


def side_kernel(ids_ref, logits_ref, stats_ref, full_ref, half_ref, loss_ref):
    tok, experts = logits_ref.shape
    devices = stats_ref.shape[0] // 8
    stats = jnp.sum(stats_ref[...].astype(F32).reshape(devices, 8, experts), axis=0)
    total_probs = stats[1:2] + (stats[2:3] + stats[3:4])
    tokens_all = tok * devices
    share = stats[0:1] / (tokens_all * ids_ref.shape[0]) * (total_probs / tokens_all)
    loss_ref[0, 0] = experts * jnp.sum(share)
    hit, slots = slots_by_expert(ids_ref, experts)
    hit = hit.T
    slots = slots.T
    chosen = jnp.where(hit > 0.0, probabilities(logits_ref[...]), 0.0)
    weights = chosen / jnp.sum(chosen, axis=1, keepdims=True)
    columns = experts * 8
    spread = jnp.where(iota((experts, columns), 1) // 8 == iota((experts, columns), 0), 1.0, 0.0).astype(BF)
    wide = dot(slots.astype(BF), spread)
    line = iota(wide.shape, 1) % 8
    in_full = wide == line.astype(F32)
    in_half = wide == (FULL + line % HALF).astype(F32)
    for number, term in enumerate(three_terms(weights)[:2]):
        value = dot(term, spread)
        rows = slice(number * tok, (number + 1) * tok)
        full_ref[rows, :] = jnp.where(in_full, value, 0.0).astype(BF)
        half_ref[0, rows, :] = jnp.where(in_half & (line < HALF), value, 0.0).astype(BF)
        half_ref[1, rows, :] = jnp.where(in_half & (line >= HALF), value, 0.0).astype(BF)


def add_terms(product):
    tok = product.shape[0] // 2
    return product[:tok] + product[tok:]


def sum_kernel(full_weights_ref, half_weights_ref, full_ref, half_ref, out_ref):
    step = pl.program_id(0)
    lanes = out_ref.shape[1]
    steps = half_ref.shape[1] // lanes
    side = step // steps
    full = full_ref[:, pl.ds(pl.multiple_of(step * lanes, lanes), lanes)]
    half = half_ref[:, pl.ds(pl.multiple_of((step - side * steps) * lanes, lanes), lanes)]
    total = dot(full_weights_ref[...], full) + dot(half_weights_ref[side], half)
    out_ref[...] = add_terms(total).astype(BF)


def whole(shape):
    zeros = (0,) * len(shape)
    return pl.BlockSpec(shape, lambda *_: zeros, pipeline_mode=pl.Buffered(1))


def call(kernel, grid, out_shape, in_specs, out_specs, flops, moved, limit=20, scratch=()):
    return pl.pallas_call(
        kernel,
        grid=grid,
        out_shape=out_shape,
        in_specs=in_specs,
        out_specs=out_specs,
        scratch_shapes=scratch,
        name=kernel.__name__,
        cost_estimate=pl.CostEstimate(flops=flops, bytes_accessed=moved, transcendentals=0),
        compiler_params=pltpu.CompilerParams(
            dimension_semantics=("arbitrary",) * len(grid), vmem_limit_bytes=limit * 2**20
        ),
    )


def local(tokens, router_logits, expert_ids, w_gate, w_up, w_down):
    tok, top_k = expert_ids.shape
    width = tokens.shape[1]
    experts = router_logits.shape[1]
    ff = w_gate.shape[2]
    devices = lax.axis_size(ROW_COL)
    half = width // 2
    lines = experts * 8
    ids = expert_ids.T
    in_vmem = lambda x: pltpu.with_memory_space_constraint(x, pltpu.VMEM)
    in_hbm = lambda x: pltpu.with_memory_space_constraint(x, pltpu.HBM)
    resident = pl.BlockSpec(memory_space=pltpu.VMEM)
    gate, up, down = in_vmem(w_gate[0]), in_vmem(w_up[0]), in_vmem(w_down[0])
    shape = jax.ShapeDtypeStruct

    def exchange(x):
        lanes = x.shape[1]
        moved = lax.all_to_all(
            x.reshape(experts, 8, lanes), ROW_COL, split_axis=0, concat_axis=0, tiled=True
        )
        return moved.reshape(lines, lanes)

    sent = width + half + experts
    send = call(
        send_kernel,
        (),
        pltpu.VMEM((lines, sent), BF),
        [whole(ids.shape), whole(router_logits.shape), pl.BlockSpec(memory_space=pltpu.HBM)],
        resident,
        2 * lines * tok * (width + 2 * half),
        2 * lines * sent,
        scratch=(pltpu.VMEM(tokens.shape, BF), pltpu.SemaphoreType.DMA),
    )(in_hbm(ids), in_hbm(router_logits), in_hbm(tokens))
    got = exchange(send)
    made_half = call(
        ffn_half_kernel,
        (2,),
        pltpu.HBM((lines, half), BF),
        [pl.BlockSpec((lines // 2, half), lambda i: (i, 2))] + [resident] * 3,
        pl.BlockSpec((lines // 2, half), lambda i: (i, 0)),
        3 * lines * width * ff,
        2 * lines * width + 6 * width * ff,
        30,
    )(got, gate, up, down)
    back_half = exchange(made_half)
    weights_full, weights_half, loss = call(
        side_kernel,
        (1,),
        (
            shape((2 * tok, lines), BF),
            shape((2, 2 * tok, lines), BF),
            shape((1, 1), F32),
        ),
        [
            whole(ids.shape),
            whole(router_logits.shape),
            pl.BlockSpec((lines, experts), lambda i: (0, (width + half) // experts)),
        ],
        (
            whole((2 * tok, lines)),
            whole((2, 2 * tok, lines)),
            pl.BlockSpec(memory_space=pltpu.SMEM),
        ),
        6 * tok * experts * lines,
        12 * tok * lines,
    )(ids, router_logits, got)
    made_full = call(
        ffn_full_kernel,
        (4,),
        pltpu.VMEM((lines, width), BF),
        [
            pl.BlockSpec(memory_space=pl.ANY),
            pl.BlockSpec((lines // 4, width), lambda i: (i, 0)),
        ]
        + [resident] * 3,
        resident,
        6 * lines * width * ff,
        4 * lines * width + 6 * width * ff,
        24,
    )(weights_full, got, gate, up, down)
    back_full = exchange(made_full)

    lanes = half // 4
    mixed = call(
        sum_kernel,
        (8,),
        shape((tok, width), BF),
        [resident] * 4,
        pl.BlockSpec((tok, lanes), lambda i: (0, i)),
        8 * tok * lines * width,
        2 * lines * (width + half),
    )(in_vmem(weights_full), in_vmem(weights_half), in_vmem(back_full), in_vmem(back_half))
    return mixed, loss.reshape(())


def solution(mesh):
    torus = Mesh(mesh.devices.reshape(4, 2, 4, 4), ROW_COL)
    rows = P(ROW_COL, None)
    expert = P(ROW_COL, None, None)
    return jax.shard_map(
        local,
        mesh=torus,
        in_specs=(rows, rows, rows, expert, expert, expert),
        out_specs=(rows, P()),
        check_vma=False,
    )
```

```python
import functools

import jax
import jax.numpy as jnp
from jax import lax
from jax.experimental import pallas as pl
from jax.experimental.pallas import tpu as pltpu
from jax.sharding import Mesh
from jax.sharding import PartitionSpec as P

ROW_COL = ("row_0", "row_1", "col_0", "col_1")
BF = jnp.bfloat16
F32 = jnp.float32
NONE = 255.0
FULL = 8
HALF = 4


def iota(shape, dim):
    return lax.broadcasted_iota(jnp.int32, shape, dim)


def dot(a, b):
    return lax.dot_general(a, b, (((1,), (0,)), ((), ())), preferred_element_type=F32)


def chosen_by_expert(ids_ref, experts):
    top_k, tok = ids_ref.shape
    rows = iota((experts, tok), 0)
    hit = jnp.zeros((experts, tok), F32)
    for k in range(top_k):
        hit = hit + jnp.where(rows == ids_ref[k : k + 1, :], 1.0, 0.0)
    return hit


def slots_by_expert(ids_ref, experts):
    tok = ids_ref.shape[1]
    hit = chosen_by_expert(ids_ref, experts)
    before = jnp.where(iota((tok, tok), 0) < iota((tok, tok), 1), 1.0, 0.0).astype(BF)
    earlier = dot(hit.astype(BF), before)
    return hit, jnp.where(hit > 0.0, earlier, NONE)


def probabilities(logits):
    shifted = jnp.exp(logits - jnp.max(logits, axis=1, keepdims=True))
    return shifted / jnp.sum(shifted, axis=1, keepdims=True)


def three_terms(x):
    high = x.astype(BF)
    rest = x - high.astype(F32)
    mid = rest.astype(BF)
    low = (rest - mid.astype(F32)).astype(BF)
    return high, mid, low


def spread_rows(slots, step, rows, experts):
    pick = iota((rows, experts), 0) // 8 + step * (rows // 8) == iota((rows, experts), 1)
    return dot(jnp.where(pick, 1.0, 0.0).astype(BF), slots)


def send_kernel(ids_ref, logits_ref, hbm_ref, out_ref, tok_ref, arrived):
    tok, width = hbm_ref.shape
    experts = logits_ref.shape[1]
    half = width // 2
    fetches = [
        pltpu.make_async_copy(
            hbm_ref.at[:, side * half : (side + 1) * half],
            tok_ref.at[side * tok : (side + 1) * tok],
            arrived.at[side],
        )
        for side in range(2)
    ]
    for fetch in fetches:
        fetch.start()
    hit, slots = slots_by_expert(ids_ref, experts)
    slots = slots.astype(BF)
    counts = jnp.sum(hit.T, axis=0, keepdims=True)
    sums = jnp.sum(probabilities(logits_ref[...]), axis=0, keepdims=True)
    line = iota((8, experts), 0)
    tile = jnp.where(line == 0, counts, 0.0)
    for number, term in enumerate(three_terms(sums)):
        tile = jnp.where(line == number + 1, term.astype(F32), tile)
    rows = 256
    stats = jnp.broadcast_to(tile[None], (rows // 8, 8, experts)).reshape(rows, experts).astype(BF)
    for fetch in fetches:
        fetch.wait()
    for step in range(experts * 8 // rows):
        at = slice(step * rows, (step + 1) * rows)
        wide = spread_rows(slots, step, rows, experts)
        line = iota(wide.shape, 0) % 8
        full = jnp.where(wide == line.astype(F32), 1.0, 0.0).astype(BF)
        out_ref[at, :half] = dot(full, tok_ref[:tok]).astype(BF)
        out_ref[at, half:width] = dot(full, tok_ref[tok:]).astype(BF)
        match = wide == (FULL + line % HALF).astype(F32)
        first = jnp.where(match & (line < HALF), 1.0, 0.0).astype(BF)
        second = jnp.where(match & (line >= HALF), 1.0, 0.0).astype(BF)
        both = jnp.concatenate([first, second], axis=1)
        out_ref[at, width : width + half] = dot(both, tok_ref[...]).astype(BF)
        out_ref[at, width + half :] = stats


def silu_times(gate, up):
    return gate * (1.0 / (1.0 + jnp.exp(-gate))) * up


def ffn_full_kernel(after_ref, x_ref, gate_ref, up_ref, down_ref, out_ref):
    x = x_ref[...]
    hidden = silu_times(dot(x, gate_ref[...]), dot(x, up_ref[...])).astype(BF)
    out_ref[...] = dot(hidden, down_ref[...]).astype(BF)


def swap_halves(first, second):
    low = iota(first.shape, 1) < HALF
    return (
        jnp.where(low, first, pltpu.roll(second, HALF, 1)),
        jnp.where(low, pltpu.roll(first, HALF, 1), second),
    )


def ffn_half_kernel(x_ref, gate_ref, up_ref, down_ref, out_ref):
    lines, half = x_ref.shape
    pairs = x_ref[...].astype(F32).reshape(lines // 16, 2, 8, half)
    first, second = swap_halves(pairs[:, 0], pairs[:, 1])
    first = first.reshape(lines // 2, half).astype(BF)
    second = second.reshape(lines // 2, half).astype(BF)
    gate = dot(first, gate_ref[:half]) + dot(second, gate_ref[half:])
    up = dot(first, up_ref[:half]) + dot(second, up_ref[half:])
    hidden = silu_times(gate, up).astype(BF)
    tiles = (lines // 16, 8, half)
    first = dot(hidden, down_ref[:, :half]).reshape(tiles)
    second = dot(hidden, down_ref[:, half:]).reshape(tiles)
    first, second = swap_halves(first, second)
    out_ref[...] = jnp.stack([first, second], axis=1).reshape(lines, half).astype(BF)


def side_kernel(ids_ref, logits_ref, stats_ref, full_ref, half_ref, loss_ref):
    tok, experts = logits_ref.shape
    devices = stats_ref.shape[0] // 8
    stats = jnp.sum(stats_ref[...].astype(F32).reshape(devices, 8, experts), axis=0)
    total_probs = stats[1:2] + (stats[2:3] + stats[3:4])
    tokens_all = tok * devices
    share = stats[0:1] / (tokens_all * ids_ref.shape[0]) * (total_probs / tokens_all)
    loss_ref[0, 0] = experts * jnp.sum(share)
    hit, slots = slots_by_expert(ids_ref, experts)
    hit = hit.T
    slots = slots.T
    chosen = jnp.where(hit > 0.0, probabilities(logits_ref[...]), 0.0)
    weights = chosen / jnp.sum(chosen, axis=1, keepdims=True)
    columns = experts * 8
    spread = jnp.where(iota((experts, columns), 1) // 8 == iota((experts, columns), 0), 1.0, 0.0).astype(BF)
    wide = dot(slots.astype(BF), spread)
    line = iota(wide.shape, 1) % 8
    in_full = wide == line.astype(F32)
    in_half = wide == (FULL + line % HALF).astype(F32)
    for number, term in enumerate(three_terms(weights)[:2]):
        value = dot(term, spread)
        rows = slice(number * tok, (number + 1) * tok)
        full_ref[rows, :] = jnp.where(in_full, value, 0.0).astype(BF)
        half_ref[0, rows, :] = jnp.where(in_half & (line < HALF), value, 0.0).astype(BF)
        half_ref[1, rows, :] = jnp.where(in_half & (line >= HALF), value, 0.0).astype(BF)


def add_terms(product):
    tok = product.shape[0] // 2
    return product[:tok] + product[tok:]


def sum_kernel(full_weights_ref, half_weights_ref, full_ref, half_ref, out_ref):
    side = pl.program_id(1)
    lanes = out_ref.shape[1]
    start = (side * pl.num_programs(0) + pl.program_id(0)) * lanes
    full = full_ref[:, pl.ds(pl.multiple_of(start, lanes), lanes)]
    total = dot(full_weights_ref[...], full) + dot(half_weights_ref[side], half_ref[...])
    out_ref[...] = add_terms(total).astype(BF)


def whole(shape):
    zeros = (0,) * len(shape)
    return pl.BlockSpec(shape, lambda *_: zeros, pipeline_mode=pl.Buffered(1))


def call(kernel, grid, out_shape, in_specs, out_specs, flops, moved, limit=20, scratch=()):
    return pl.pallas_call(
        kernel,
        grid=grid,
        out_shape=out_shape,
        in_specs=in_specs,
        out_specs=out_specs,
        scratch_shapes=scratch,
        name=kernel.__name__,
        cost_estimate=pl.CostEstimate(flops=flops, bytes_accessed=moved, transcendentals=0),
        compiler_params=pltpu.CompilerParams(
            dimension_semantics=("arbitrary",) * len(grid), vmem_limit_bytes=limit * 2**20
        ),
    )


def local(tokens, router_logits, expert_ids, w_gate, w_up, w_down):
    tok, top_k = expert_ids.shape
    width = tokens.shape[1]
    experts = router_logits.shape[1]
    ff = w_gate.shape[2]
    devices = lax.axis_size(ROW_COL)
    half = width // 2
    lines = experts * 8
    ids = expert_ids.T
    in_vmem = lambda x: pltpu.with_memory_space_constraint(x, pltpu.VMEM)
    in_hbm = lambda x: pltpu.with_memory_space_constraint(x, pltpu.HBM)
    resident = pl.BlockSpec(memory_space=pltpu.VMEM)
    gate, up, down = in_vmem(w_gate[0]), in_vmem(w_up[0]), in_vmem(w_down[0])
    shape = jax.ShapeDtypeStruct

    def exchange(x):
        lanes = x.shape[1]
        moved = lax.all_to_all(
            x.reshape(experts, 8, lanes), ROW_COL, split_axis=0, concat_axis=0, tiled=True
        )
        return moved.reshape(lines, lanes)

    sent = width + half + experts
    send = call(
        send_kernel,
        (),
        pltpu.VMEM((lines, sent), BF),
        [whole(ids.shape), whole(router_logits.shape), pl.BlockSpec(memory_space=pltpu.HBM)],
        resident,
        2 * lines * tok * (width + 2 * half),
        2 * lines * sent,
        scratch=(pltpu.VMEM((2 * tok, half), BF), pltpu.SemaphoreType.DMA((2,))),
    )(in_hbm(ids), in_hbm(router_logits), in_hbm(tokens))
    got = in_hbm(exchange(send))
    made_half = call(
        ffn_half_kernel,
        (2,),
        pltpu.HBM((lines, half), BF),
        [pl.BlockSpec((lines // 2, half), lambda i: (i, 2))] + [resident] * 3,
        pl.BlockSpec((lines // 2, half), lambda i: (i, 0)),
        3 * lines * width * ff,
        2 * lines * width + 6 * width * ff,
        30,
    )(got, gate, up, down)
    back_half = exchange(made_half)
    weights_full, weights_half, loss = call(
        side_kernel,
        (1,),
        (
            shape((2 * tok, lines), BF),
            shape((2, 2 * tok, lines), BF),
            shape((1, 1), F32),
        ),
        [
            whole(ids.shape),
            whole(router_logits.shape),
            pl.BlockSpec((lines, experts), lambda i: (0, (width + half) // experts)),
        ],
        (
            whole((2 * tok, lines)),
            whole((2, 2 * tok, lines)),
            pl.BlockSpec(memory_space=pltpu.SMEM),
        ),
        6 * tok * experts * lines,
        12 * tok * lines,
    )(ids, router_logits, got)
    made_full = call(
        ffn_full_kernel,
        (4,),
        pltpu.HBM((lines, width), BF),
        [
            pl.BlockSpec(memory_space=pl.ANY),
            pl.BlockSpec((lines // 4, width), lambda i: (i, 0)),
        ]
        + [resident] * 3,
        pl.BlockSpec((lines // 4, width), lambda i: (i, 0)),
        6 * lines * width * ff,
        4 * lines * width + 6 * width * ff,
        24,
    )(weights_full, got, gate, up, down)
    back_full = exchange(made_full)

    lanes = half // 4
    mixed = call(
        sum_kernel,
        (4, 2),
        shape((tok, width), BF),
        [resident] * 3 + [pl.BlockSpec((lines, lanes), lambda i, side: (0, i))],
        pl.BlockSpec((tok, lanes), lambda i, side: (0, side * 4 + i)),
        8 * tok * lines * width,
        2 * lines * (width + half),
    )(in_vmem(weights_full), in_vmem(weights_half), in_vmem(back_full), in_hbm(back_half))
    return mixed, loss.reshape(())


def solution(mesh):
    torus = Mesh(mesh.devices.reshape(4, 2, 4, 4), ROW_COL)
    rows = P(ROW_COL, None)
    expert = P(ROW_COL, None, None)
    return jax.shard_map(
        local,
        mesh=torus,
        in_specs=(rows, rows, rows, expert, expert, expert),
        out_specs=(rows, P()),
        check_vma=False,
    )
```

```python
import functools

import jax
import jax.numpy as jnp
from jax import lax
from jax.experimental import pallas as pl
from jax.experimental.pallas import tpu as pltpu
from jax.sharding import Mesh
from jax.sharding import PartitionSpec as P

ROW_COL = ("row_0", "row_1", "col_0", "col_1")
BF = jnp.bfloat16
F32 = jnp.float32
NONE = 255.0
FULL = 8
HALF = 4


def iota(shape, dim):
    return lax.broadcasted_iota(jnp.int32, shape, dim)


def dot(a, b):
    return lax.dot_general(a, b, (((1,), (0,)), ((), ())), preferred_element_type=F32)


def chosen_by_expert(ids_ref, experts):
    top_k, tok = ids_ref.shape
    rows = iota((experts, tok), 0)
    hit = jnp.zeros((experts, tok), F32)
    for k in range(top_k):
        hit = hit + jnp.where(rows == ids_ref[k : k + 1, :], 1.0, 0.0)
    return hit


def slots_by_expert(ids_ref, experts):
    tok = ids_ref.shape[1]
    hit = chosen_by_expert(ids_ref, experts)
    before = jnp.where(iota((tok, tok), 0) < iota((tok, tok), 1), 1.0, 0.0).astype(BF)
    earlier = dot(hit.astype(BF), before)
    return hit, jnp.where(hit > 0.0, earlier, NONE)


def probabilities(logits):
    shifted = jnp.exp(logits - jnp.max(logits, axis=1, keepdims=True))
    return shifted / jnp.sum(shifted, axis=1, keepdims=True)


def three_terms(x):
    high = x.astype(BF)
    rest = x - high.astype(F32)
    mid = rest.astype(BF)
    low = (rest - mid.astype(F32)).astype(BF)
    return high, mid, low


def spread_rows(slots, step, rows, experts):
    pick = iota((rows, experts), 0) // 8 + step * (rows // 8) == iota((rows, experts), 1)
    return dot(jnp.where(pick, 1.0, 0.0).astype(BF), slots)


def send_kernel(ids_ref, logits_ref, hbm_ref, out_ref, tok_ref, arrived):
    tok, width = hbm_ref.shape
    experts = logits_ref.shape[1]
    half = width // 2
    fetches = [
        pltpu.make_async_copy(
            hbm_ref.at[:, side * half : (side + 1) * half],
            tok_ref.at[side * tok : (side + 1) * tok],
            arrived.at[side],
        )
        for side in range(2)
    ]
    for fetch in fetches:
        fetch.start()
    hit, slots = slots_by_expert(ids_ref, experts)
    slots = slots.astype(BF)
    counts = jnp.sum(hit.T, axis=0, keepdims=True)
    sums = jnp.sum(probabilities(logits_ref[...]), axis=0, keepdims=True)
    line = iota((8, experts), 0)
    tile = jnp.where(line == 0, counts, 0.0)
    for number, term in enumerate(three_terms(sums)):
        tile = jnp.where(line == number + 1, term.astype(F32), tile)
    rows = 256
    stats = jnp.broadcast_to(tile[None], (rows // 8, 8, experts)).reshape(rows, experts).astype(BF)
    for fetch in fetches:
        fetch.wait()
    for step in range(experts * 8 // rows):
        at = slice(step * rows, (step + 1) * rows)
        wide = spread_rows(slots, step, rows, experts)
        line = iota(wide.shape, 0) % 8
        full = jnp.where(wide == line.astype(F32), 1.0, 0.0).astype(BF)
        out_ref[at, :half] = dot(full, tok_ref[:tok]).astype(BF)
        out_ref[at, half:width] = dot(full, tok_ref[tok:]).astype(BF)
        match = wide == (FULL + line % HALF).astype(F32)
        first = jnp.where(match & (line < HALF), 1.0, 0.0).astype(BF)
        second = jnp.where(match & (line >= HALF), 1.0, 0.0).astype(BF)
        both = jnp.concatenate([first, second], axis=1)
        out_ref[at, width : width + half] = dot(both, tok_ref[...]).astype(BF)
        out_ref[at, width + half :] = stats


def silu_times(gate, up):
    return gate * (1.0 / (1.0 + jnp.exp(-gate))) * up


def ffn_full_kernel(after_ref, x_ref, gate_ref, up_ref, down_ref, out_ref):
    x = x_ref[...]
    hidden = silu_times(dot(x, gate_ref[...]), dot(x, up_ref[...])).astype(BF)
    out_ref[...] = dot(hidden, down_ref[...]).astype(BF)


def swap_halves(first, second):
    low = iota(first.shape, 1) < HALF
    return (
        jnp.where(low, first, pltpu.roll(second, HALF, 1)),
        jnp.where(low, pltpu.roll(first, HALF, 1), second),
    )


def ffn_half_kernel(x_ref, gate_ref, up_ref, down_ref, out_ref):
    lines, half = x_ref.shape
    pairs = x_ref[...].astype(F32).reshape(lines // 16, 2, 8, half)
    first, second = swap_halves(pairs[:, 0], pairs[:, 1])
    first = first.reshape(lines // 2, half).astype(BF)
    second = second.reshape(lines // 2, half).astype(BF)
    gate = dot(first, gate_ref[:half]) + dot(second, gate_ref[half:])
    up = dot(first, up_ref[:half]) + dot(second, up_ref[half:])
    hidden = silu_times(gate, up).astype(BF)
    tiles = (lines // 16, 8, half)
    first = dot(hidden, down_ref[:, :half]).reshape(tiles)
    second = dot(hidden, down_ref[:, half:]).reshape(tiles)
    first, second = swap_halves(first, second)
    out_ref[...] = jnp.stack([first, second], axis=1).reshape(lines, half).astype(BF)


def side_kernel(ids_ref, logits_ref, stats_ref, full_ref, half_ref, loss_ref):
    tok, experts = logits_ref.shape
    devices = stats_ref.shape[0] // 8
    stats = jnp.sum(stats_ref[...].astype(F32).reshape(devices, 8, experts), axis=0)
    total_probs = stats[1:2] + (stats[2:3] + stats[3:4])
    tokens_all = tok * devices
    share = stats[0:1] / (tokens_all * ids_ref.shape[0]) * (total_probs / tokens_all)
    loss_ref[0, 0] = experts * jnp.sum(share)
    hit, slots = slots_by_expert(ids_ref, experts)
    hit = hit.T
    slots = slots.T
    chosen = jnp.where(hit > 0.0, probabilities(logits_ref[...]), 0.0)
    weights = chosen / jnp.sum(chosen, axis=1, keepdims=True)
    columns = experts * 8
    spread = jnp.where(iota((experts, columns), 1) // 8 == iota((experts, columns), 0), 1.0, 0.0).astype(BF)
    wide = dot(slots.astype(BF), spread)
    line = iota(wide.shape, 1) % 8
    in_full = wide == line.astype(F32)
    in_half = wide == (FULL + line % HALF).astype(F32)
    for number, term in enumerate(three_terms(weights)[:2]):
        value = dot(term, spread)
        rows = slice(number * tok, (number + 1) * tok)
        full_ref[rows, :] = jnp.where(in_full, value, 0.0).astype(BF)
        half_ref[rows, :] = jnp.where(in_half & (line < HALF), value, 0.0).astype(BF)
        rows = slice((number + 2) * tok, (number + 3) * tok)
        half_ref[rows, :] = jnp.where(in_half & (line >= HALF), value, 0.0).astype(BF)


def add_terms(product):
    tok = product.shape[0] // 2
    return product[:tok] + product[tok:]


def sum_kernel(full_weights_ref, half_weights_ref, full_ref, hbm_ref, out_ref, half_ref, made_ref, arrived, left):
    blocks, _, lanes = half_ref.shape
    half = blocks * lanes
    fetches = [
        pltpu.make_async_copy(
            hbm_ref.at[:, i * lanes : (i + 1) * lanes], half_ref.at[i], arrived.at[i]
        )
        for i in range(blocks)
    ]
    for fetch in fetches:
        fetch.start()
    sends = []
    for i, fetch in enumerate(fetches):
        places = [slice(side * half + i * lanes, side * half + (i + 1) * lanes) for side in range(2)]
        totals = [dot(full_weights_ref[...], full_ref[:, at]) for at in places]
        fetch.wait()
        rest = dot(half_weights_ref[...], half_ref[i])
        rows = rest.shape[0] // 2
        for side, at in enumerate(places):
            total = totals[side] + rest[side * rows : (side + 1) * rows]
            made_ref[:, at] = add_terms(total).astype(BF)
            send = pltpu.make_async_copy(
                made_ref.at[:, at], out_ref.at[:, at], left.at[2 * i + side]
            )
            send.start()
            sends.append(send)
    for send in sends:
        send.wait()


def whole(shape):
    zeros = (0,) * len(shape)
    return pl.BlockSpec(shape, lambda *_: zeros, pipeline_mode=pl.Buffered(1))


def call(kernel, grid, out_shape, in_specs, out_specs, flops, moved, limit=20, scratch=()):
    return pl.pallas_call(
        kernel,
        grid=grid,
        out_shape=out_shape,
        in_specs=in_specs,
        out_specs=out_specs,
        scratch_shapes=scratch,
        name=kernel.__name__,
        cost_estimate=pl.CostEstimate(flops=flops, bytes_accessed=moved, transcendentals=0),
        compiler_params=pltpu.CompilerParams(
            dimension_semantics=("arbitrary",) * len(grid), vmem_limit_bytes=limit * 2**20
        ),
    )


def local(tokens, router_logits, expert_ids, w_gate, w_up, w_down):
    tok, top_k = expert_ids.shape
    width = tokens.shape[1]
    experts = router_logits.shape[1]
    ff = w_gate.shape[2]
    devices = lax.axis_size(ROW_COL)
    half = width // 2
    lines = experts * 8
    ids = expert_ids.T
    in_vmem = lambda x: pltpu.with_memory_space_constraint(x, pltpu.VMEM)
    in_hbm = lambda x: pltpu.with_memory_space_constraint(x, pltpu.HBM)
    resident = pl.BlockSpec(memory_space=pltpu.VMEM)
    gate, up, down = in_vmem(w_gate[0]), in_vmem(w_up[0]), in_vmem(w_down[0])
    shape = jax.ShapeDtypeStruct

    def exchange(x):
        lanes = x.shape[1]
        moved = lax.all_to_all(
            x.reshape(experts, 8, lanes), ROW_COL, split_axis=0, concat_axis=0, tiled=True
        )
        return moved.reshape(lines, lanes)

    sent = width + half + experts
    send = call(
        send_kernel,
        (),
        pltpu.VMEM((lines, sent), BF),
        [whole(ids.shape), whole(router_logits.shape), pl.BlockSpec(memory_space=pltpu.HBM)],
        resident,
        2 * lines * tok * (width + 2 * half),
        2 * lines * sent,
        scratch=(pltpu.VMEM((2 * tok, half), BF), pltpu.SemaphoreType.DMA((2,))),
    )(in_hbm(ids), in_hbm(router_logits), in_hbm(tokens))
    got = in_hbm(exchange(send))
    made_half = call(
        ffn_half_kernel,
        (2,),
        pltpu.HBM((lines, half), BF),
        [pl.BlockSpec((lines // 2, half), lambda i: (i, 2))] + [resident] * 3,
        pl.BlockSpec((lines // 2, half), lambda i: (i, 0)),
        3 * lines * width * ff,
        2 * lines * width + 6 * width * ff,
        30,
    )(got, gate, up, down)
    back_half = exchange(made_half)
    weights_full, weights_half, loss = call(
        side_kernel,
        (1,),
        (
            shape((2 * tok, lines), BF),
            shape((4 * tok, lines), BF),
            shape((1, 1), F32),
        ),
        [
            whole(ids.shape),
            whole(router_logits.shape),
            pl.BlockSpec((lines, experts), lambda i: (0, (width + half) // experts)),
        ],
        (
            whole((2 * tok, lines)),
            whole((4 * tok, lines)),
            pl.BlockSpec(memory_space=pltpu.SMEM),
        ),
        6 * tok * experts * lines,
        12 * tok * lines,
    )(ids, router_logits, got)
    made_full = call(
        ffn_full_kernel,
        (4,),
        pltpu.HBM((lines, width), BF),
        [
            pl.BlockSpec(memory_space=pl.ANY),
            pl.BlockSpec((lines // 4, width), lambda i: (i, 0)),
        ]
        + [resident] * 3,
        pl.BlockSpec((lines // 4, width), lambda i: (i, 0)),
        6 * lines * width * ff,
        4 * lines * width + 6 * width * ff,
        24,
    )(weights_full, got, gate, up, down)
    back_full = exchange(made_full)

    lanes = half // 4
    in_place = pl.BlockSpec(memory_space=pltpu.HBM)
    mixed = call(
        sum_kernel,
        (),
        pltpu.HBM((tok, width), BF),
        [resident] * 3 + [in_place],
        in_place,
        8 * tok * lines * width,
        2 * lines * (width + half),
        scratch=(
            pltpu.VMEM((4, lines, lanes), BF),
            pltpu.VMEM((tok, width), BF),
            pltpu.SemaphoreType.DMA((4,)),
            pltpu.SemaphoreType.DMA((8,)),
        ),
    )(in_vmem(weights_full), in_vmem(weights_half), in_vmem(back_full), in_hbm(back_half))
    return mixed, loss.reshape(())


def solution(mesh):
    torus = Mesh(mesh.devices.reshape(4, 2, 4, 4), ROW_COL)
    rows = P(ROW_COL, None)
    expert = P(ROW_COL, None, None)
    return jax.shard_map(
        local,
        mesh=torus,
        in_specs=(rows, rows, rows, expert, expert, expert),
        out_specs=(rows, P()),
        check_vma=False,
    )
```

```python
import functools

import jax
import jax.numpy as jnp
from jax import lax
from jax.experimental import pallas as pl
from jax.experimental.pallas import tpu as pltpu
from jax.sharding import Mesh
from jax.sharding import PartitionSpec as P

ROW_COL = ("row_0", "row_1", "col_0", "col_1")
BF = jnp.bfloat16
F32 = jnp.float32
NONE = 255.0
FULL = 8
HALF = 4


def iota(shape, dim):
    return lax.broadcasted_iota(jnp.int32, shape, dim)


def dot(a, b):
    return lax.dot_general(a, b, (((1,), (0,)), ((), ())), preferred_element_type=F32)


def chosen_by_expert(ids_ref, experts):
    top_k, tok = ids_ref.shape
    rows = iota((experts, tok), 0)
    hit = jnp.zeros((experts, tok), F32)
    for k in range(top_k):
        hit = hit + jnp.where(rows == ids_ref[k : k + 1, :], 1.0, 0.0)
    return hit


def slots_by_expert(ids_ref, experts):
    tok = ids_ref.shape[1]
    hit = chosen_by_expert(ids_ref, experts)
    before = jnp.where(iota((tok, tok), 0) < iota((tok, tok), 1), 1.0, 0.0).astype(BF)
    earlier = dot(hit.astype(BF), before)
    return hit, jnp.where(hit > 0.0, earlier, NONE)


def probabilities(logits):
    shifted = jnp.exp(logits - jnp.max(logits, axis=1, keepdims=True))
    return shifted / jnp.sum(shifted, axis=1, keepdims=True)


def three_terms(x):
    high = x.astype(BF)
    rest = x - high.astype(F32)
    mid = rest.astype(BF)
    low = (rest - mid.astype(F32)).astype(BF)
    return high, mid, low


def spread_rows(slots, step, rows, experts):
    pick = iota((rows, experts), 0) // 8 + step * (rows // 8) == iota((rows, experts), 1)
    return dot(jnp.where(pick, 1.0, 0.0).astype(BF), slots)


def send_kernel(ids_hbm, logits_hbm, hbm_ref, out_ref, ids_ref, logits_ref, tok_ref, arrived):
    tok, width = hbm_ref.shape
    experts = logits_ref.shape[1]
    half = width // 2
    fetches = [
        pltpu.make_async_copy(
            hbm_ref.at[:, side * half : (side + 1) * half],
            tok_ref.at[side * tok : (side + 1) * tok],
            arrived.at[side],
        )
        for side in range(2)
    ]
    ids_fetch = pltpu.make_async_copy(ids_hbm, ids_ref, arrived.at[2])
    logits_fetch = pltpu.make_async_copy(logits_hbm, logits_ref, arrived.at[3])
    for fetch in [ids_fetch] + fetches + [logits_fetch]:
        fetch.start()
    ids_fetch.wait()
    hit, slots = slots_by_expert(ids_ref, experts)
    slots = slots.astype(BF)
    rows = 256
    for fetch in fetches + [logits_fetch]:
        fetch.wait()
    counts = jnp.sum(hit.T, axis=0, keepdims=True)
    sums = jnp.sum(probabilities(logits_ref[...]), axis=0, keepdims=True)
    line = iota((8, experts), 0)
    tile = jnp.where(line == 0, counts, 0.0)
    for number, term in enumerate(three_terms(sums)):
        tile = jnp.where(line == number + 1, term.astype(F32), tile)
    stats = jnp.broadcast_to(tile[None], (rows // 8, 8, experts)).reshape(rows, experts).astype(BF)
    for step in range(experts * 8 // rows):
        at = slice(step * rows, (step + 1) * rows)
        wide = spread_rows(slots, step, rows, experts)
        line = iota(wide.shape, 0) % 8
        full = jnp.where(wide == line.astype(F32), 1.0, 0.0).astype(BF)
        out_ref[at, :half] = dot(full, tok_ref[:tok]).astype(BF)
        out_ref[at, half:width] = dot(full, tok_ref[tok:]).astype(BF)
        match = wide == (FULL + line % HALF).astype(F32)
        first = jnp.where(match & (line < HALF), 1.0, 0.0).astype(BF)
        second = jnp.where(match & (line >= HALF), 1.0, 0.0).astype(BF)
        both = jnp.concatenate([first, second], axis=1)
        out_ref[at, width : width + half] = dot(both, tok_ref[...]).astype(BF)
        out_ref[at, width + half :] = stats


def silu_times(gate, up):
    return gate * (1.0 / (1.0 + jnp.exp(-gate))) * up


def ffn_full_kernel(after_ref, x_ref, gate_ref, up_ref, down_ref, out_ref):
    x = x_ref[...]
    hidden = silu_times(dot(x, gate_ref[...]), dot(x, up_ref[...])).astype(BF)
    out_ref[...] = dot(hidden, down_ref[...]).astype(BF)


def swap_halves(first, second):
    low = iota(first.shape, 1) < HALF
    return (
        jnp.where(low, first, pltpu.roll(second, HALF, 1)),
        jnp.where(low, pltpu.roll(first, HALF, 1), second),
    )


def ffn_half_kernel(x_ref, gate_ref, up_ref, down_ref, out_ref):
    lines, half = x_ref.shape
    pairs = x_ref[...].astype(F32).reshape(lines // 16, 2, 8, half)
    first, second = swap_halves(pairs[:, 0], pairs[:, 1])
    first = first.reshape(lines // 2, half).astype(BF)
    second = second.reshape(lines // 2, half).astype(BF)
    gate = dot(first, gate_ref[:half]) + dot(second, gate_ref[half:])
    up = dot(first, up_ref[:half]) + dot(second, up_ref[half:])
    hidden = silu_times(gate, up).astype(BF)
    tiles = (lines // 16, 8, half)
    first = dot(hidden, down_ref[:, :half]).reshape(tiles)
    second = dot(hidden, down_ref[:, half:]).reshape(tiles)
    first, second = swap_halves(first, second)
    out_ref[...] = jnp.stack([first, second], axis=1).reshape(lines, half).astype(BF)


def side_kernel(ids_ref, logits_ref, stats_ref, full_ref, half_ref, loss_ref):
    tok, experts = logits_ref.shape
    devices = stats_ref.shape[0] // 8
    stats = jnp.sum(stats_ref[...].astype(F32).reshape(devices, 8, experts), axis=0)
    total_probs = stats[1:2] + (stats[2:3] + stats[3:4])
    tokens_all = tok * devices
    share = stats[0:1] / (tokens_all * ids_ref.shape[0]) * (total_probs / tokens_all)
    loss_ref[0, 0] = experts * jnp.sum(share)
    hit, slots = slots_by_expert(ids_ref, experts)
    hit = hit.T
    slots = slots.T
    chosen = jnp.where(hit > 0.0, probabilities(logits_ref[...]), 0.0)
    weights = chosen / jnp.sum(chosen, axis=1, keepdims=True)
    columns = experts * 8
    spread = jnp.where(iota((experts, columns), 1) // 8 == iota((experts, columns), 0), 1.0, 0.0).astype(BF)
    wide = dot(slots.astype(BF), spread)
    line = iota(wide.shape, 1) % 8
    in_full = wide == line.astype(F32)
    in_half = wide == (FULL + line % HALF).astype(F32)
    for number, term in enumerate(three_terms(weights)[:2]):
        value = dot(term, spread)
        rows = slice(number * tok, (number + 1) * tok)
        full_ref[rows, :] = jnp.where(in_full, value, 0.0).astype(BF)
        half_ref[rows, :] = jnp.where(in_half & (line < HALF), value, 0.0).astype(BF)
        rows = slice((number + 2) * tok, (number + 3) * tok)
        half_ref[rows, :] = jnp.where(in_half & (line >= HALF), value, 0.0).astype(BF)


def add_terms(product):
    tok = product.shape[0] // 2
    return product[:tok] + product[tok:]


def sum_kernel(full_weights_ref, half_weights_ref, full_ref, hbm_ref, out_ref, half_ref, sofar_ref, made_ref, arrived, left):
    blocks, _, lanes = half_ref.shape
    half = blocks * lanes
    fetches = [
        pltpu.make_async_copy(
            hbm_ref.at[:, i * lanes : (i + 1) * lanes], half_ref.at[i], arrived.at[i]
        )
        for i in range(blocks)
    ]
    for fetch in fetches:
        fetch.start()
    for i in range(2 * blocks):
        at = slice(i * lanes, (i + 1) * lanes)
        sofar_ref[:, at] = add_terms(dot(full_weights_ref[...], full_ref[:, at]))
    sends = []
    for i, fetch in enumerate(fetches):
        fetch.wait()
        rest = dot(half_weights_ref[...], half_ref[i])
        rows = rest.shape[0] // 2
        for side in range(2):
            at = slice(side * half + i * lanes, side * half + (i + 1) * lanes)
            own = add_terms(rest[side * rows : (side + 1) * rows])
            made_ref[:, at] = (sofar_ref[:, at] + own).astype(BF)
            send = pltpu.make_async_copy(
                made_ref.at[:, at], out_ref.at[:, at], left.at[2 * i + side]
            )
            send.start()
            sends.append(send)
    for send in sends:
        send.wait()


def whole(shape):
    zeros = (0,) * len(shape)
    return pl.BlockSpec(shape, lambda *_: zeros, pipeline_mode=pl.Buffered(1))


def call(kernel, grid, out_shape, in_specs, out_specs, flops, moved, limit=20, scratch=()):
    return pl.pallas_call(
        kernel,
        grid=grid,
        out_shape=out_shape,
        in_specs=in_specs,
        out_specs=out_specs,
        scratch_shapes=scratch,
        name=kernel.__name__,
        cost_estimate=pl.CostEstimate(flops=flops, bytes_accessed=moved, transcendentals=0),
        compiler_params=pltpu.CompilerParams(
            dimension_semantics=("arbitrary",) * len(grid), vmem_limit_bytes=limit * 2**20
        ),
    )


def local(tokens, router_logits, expert_ids, w_gate, w_up, w_down):
    tok, top_k = expert_ids.shape
    width = tokens.shape[1]
    experts = router_logits.shape[1]
    ff = w_gate.shape[2]
    devices = lax.axis_size(ROW_COL)
    half = width // 2
    lines = experts * 8
    ids = expert_ids.T
    in_vmem = lambda x: pltpu.with_memory_space_constraint(x, pltpu.VMEM)
    in_hbm = lambda x: pltpu.with_memory_space_constraint(x, pltpu.HBM)
    resident = pl.BlockSpec(memory_space=pltpu.VMEM)
    in_place = pl.BlockSpec(memory_space=pltpu.HBM)
    gate, up, down = in_vmem(w_gate[0]), in_vmem(w_up[0]), in_vmem(w_down[0])
    shape = jax.ShapeDtypeStruct

    def exchange(x):
        lanes = x.shape[1]
        moved = lax.all_to_all(
            x.reshape(experts, 8, lanes), ROW_COL, split_axis=0, concat_axis=0, tiled=True
        )
        return moved.reshape(lines, lanes)

    sent = width + half + experts
    send = call(
        send_kernel,
        (),
        pltpu.VMEM((lines, sent), BF),
        [in_place] * 3,
        resident,
        2 * lines * tok * (width + 2 * half),
        2 * lines * sent,
        scratch=(
            pltpu.VMEM(ids.shape, jnp.int32),
            pltpu.VMEM(router_logits.shape, F32),
            pltpu.VMEM((2 * tok, half), BF),
            pltpu.SemaphoreType.DMA((4,)),
        ),
    )(in_hbm(ids), in_hbm(router_logits), in_hbm(tokens))
    got = in_hbm(exchange(send))
    made_half = call(
        ffn_half_kernel,
        (2,),
        pltpu.HBM((lines, half), BF),
        [pl.BlockSpec((lines // 2, half), lambda i: (i, 2))] + [resident] * 3,
        pl.BlockSpec((lines // 2, half), lambda i: (i, 0)),
        3 * lines * width * ff,
        2 * lines * width + 6 * width * ff,
        30,
    )(got, gate, up, down)
    back_half = exchange(made_half)
    weights_full, weights_half, loss = call(
        side_kernel,
        (1,),
        (
            shape((2 * tok, lines), BF),
            shape((4 * tok, lines), BF),
            shape((1, 1), F32),
        ),
        [
            whole(ids.shape),
            whole(router_logits.shape),
            pl.BlockSpec((lines, experts), lambda i: (0, (width + half) // experts)),
        ],
        (
            whole((2 * tok, lines)),
            whole((4 * tok, lines)),
            pl.BlockSpec(memory_space=pltpu.SMEM),
        ),
        6 * tok * experts * lines,
        12 * tok * lines,
    )(ids, router_logits, got)
    made_full = call(
        ffn_full_kernel,
        (4,),
        pltpu.HBM((lines, width), BF),
        [
            pl.BlockSpec(memory_space=pl.ANY),
            pl.BlockSpec((lines // 4, width), lambda i: (i, 0)),
        ]
        + [resident] * 3,
        pl.BlockSpec((lines // 4, width), lambda i: (i, 0)),
        6 * lines * width * ff,
        4 * lines * width + 6 * width * ff,
        24,
    )(weights_full, got, gate, up, down)
    back_full = exchange(made_full)

    lanes = half // 4
    mixed = call(
        sum_kernel,
        (),
        pltpu.HBM((tok, width), BF),
        [resident] * 3 + [in_place],
        in_place,
        8 * tok * lines * width,
        2 * lines * (width + half),
        scratch=(
            pltpu.VMEM((4, lines, lanes), BF),
            pltpu.VMEM((tok, width), F32),
            pltpu.VMEM((tok, width), BF),
            pltpu.SemaphoreType.DMA((4,)),
            pltpu.SemaphoreType.DMA((8,)),
        ),
    )(in_vmem(weights_full), in_vmem(weights_half), in_vmem(back_full), in_hbm(back_half))
    return mixed, loss.reshape(())


def solution(mesh):
    torus = Mesh(mesh.devices.reshape(4, 2, 4, 4), ROW_COL)
    rows = P(ROW_COL, None)
    expert = P(ROW_COL, None, None)
    return jax.shard_map(
        local,
        mesh=torus,
        in_specs=(rows, rows, rows, expert, expert, expert),
        out_specs=(rows, P()),
        check_vma=False,
    )
```

```python
import functools

import jax
import jax.numpy as jnp
from jax import lax
from jax.experimental import pallas as pl
from jax.experimental.pallas import tpu as pltpu
from jax.sharding import Mesh
from jax.sharding import PartitionSpec as P

ROW_COL = ("row_0", "row_1", "col_0", "col_1")
BF = jnp.bfloat16
F32 = jnp.float32
NONE = 255.0
FULL = 8
HALF = 4


def iota(shape, dim):
    return lax.broadcasted_iota(jnp.int32, shape, dim)


def dot(a, b):
    return lax.dot_general(a, b, (((1,), (0,)), ((), ())), preferred_element_type=F32)


def chosen_by_expert(ids_ref, experts):
    top_k, tok = ids_ref.shape
    rows = iota((experts, tok), 0)
    hit = jnp.zeros((experts, tok), F32)
    for k in range(top_k):
        hit = hit + jnp.where(rows == ids_ref[k : k + 1, :], 1.0, 0.0)
    return hit


def slots_by_expert(ids_ref, experts):
    tok = ids_ref.shape[1]
    hit = chosen_by_expert(ids_ref, experts)
    before = jnp.where(iota((tok, tok), 0) < iota((tok, tok), 1), 1.0, 0.0).astype(BF)
    earlier = dot(hit.astype(BF), before)
    return hit, jnp.where(hit > 0.0, earlier, NONE)


def probabilities(logits):
    shifted = jnp.exp(logits - jnp.max(logits, axis=1, keepdims=True))
    return shifted / jnp.sum(shifted, axis=1, keepdims=True)


def three_terms(x):
    high = x.astype(BF)
    rest = x - high.astype(F32)
    mid = rest.astype(BF)
    low = (rest - mid.astype(F32)).astype(BF)
    return high, mid, low


def spread_rows(slots, step, rows, experts):
    pick = iota((rows, experts), 0) // 8 + step * (rows // 8) == iota((rows, experts), 1)
    return dot(jnp.where(pick, 1.0, 0.0).astype(BF), slots)


def send_kernel(ids_hbm, logits_hbm, hbm_ref, out_ref, ids_ref, logits_ref, tok_ref, arrived):
    tok, width = hbm_ref.shape
    experts = logits_ref.shape[1]
    half = width // 2
    fetches = [
        pltpu.make_async_copy(
            hbm_ref.at[:, side * half : (side + 1) * half],
            tok_ref.at[side * tok : (side + 1) * tok],
            arrived.at[side],
        )
        for side in range(2)
    ]
    ids_fetch = pltpu.make_async_copy(ids_hbm, ids_ref, arrived.at[2])
    logits_fetch = pltpu.make_async_copy(logits_hbm, logits_ref, arrived.at[3])
    for fetch in [ids_fetch] + fetches + [logits_fetch]:
        fetch.start()
    ids_fetch.wait()
    hit, slots = slots_by_expert(ids_ref, experts)
    slots = slots.astype(BF)
    rows = 256
    for fetch in fetches + [logits_fetch]:
        fetch.wait()
    counts = jnp.sum(hit.T, axis=0, keepdims=True)
    sums = jnp.sum(probabilities(logits_ref[...]), axis=0, keepdims=True)
    line = iota((8, experts), 0)
    tile = jnp.where(line == 0, counts, 0.0)
    for number, term in enumerate(three_terms(sums)):
        tile = jnp.where(line == number + 1, term.astype(F32), tile)
    stats = jnp.broadcast_to(tile[None], (rows // 8, 8, experts)).reshape(rows, experts).astype(BF)
    for step in range(experts * 8 // rows):
        at = slice(step * rows, (step + 1) * rows)
        wide = spread_rows(slots, step, rows, experts)
        line = iota(wide.shape, 0) % 8
        full = jnp.where(wide == line.astype(F32), 1.0, 0.0).astype(BF)
        out_ref[at, :half] = dot(full, tok_ref[:tok]).astype(BF)
        out_ref[at, half:width] = dot(full, tok_ref[tok:]).astype(BF)
        match = wide == (FULL + line % HALF).astype(F32)
        first = jnp.where(match & (line < HALF), 1.0, 0.0).astype(BF)
        second = jnp.where(match & (line >= HALF), 1.0, 0.0).astype(BF)
        both = jnp.concatenate([first, second], axis=1)
        out_ref[at, width : width + half] = dot(both, tok_ref[...]).astype(BF)
        out_ref[at, width + half :] = stats


def silu_times(gate, up):
    return gate * (1.0 / (1.0 + jnp.exp(-gate))) * up


def ffn_full_kernel(after_ref, x_ref, gate_ref, up_ref, down_ref, out_ref):
    x = x_ref[...]
    hidden = silu_times(dot(x, gate_ref[...]), dot(x, up_ref[...])).astype(BF)
    out_ref[...] = dot(hidden, down_ref[...]).astype(BF)


def swap_halves(first, second):
    low = iota(first.shape, 1) < HALF
    return (
        jnp.where(low, first, pltpu.roll(second, HALF, 1)),
        jnp.where(low, pltpu.roll(first, HALF, 1), second),
    )


def ffn_half_kernel(hbm_ref, gate_ref, up_ref, down_ref, out_ref, x_ref, made_ref, arrived, left):
    lines, half = x_ref.shape
    rows = lines // 2
    blocks = [slice(i * rows, (i + 1) * rows) for i in range(2)]
    fetches = [
        pltpu.make_async_copy(hbm_ref.at[at, 2 * half : 3 * half], x_ref.at[at], arrived.at[i])
        for i, at in enumerate(blocks)
    ]
    for fetch in fetches:
        fetch.start()
    sends = []
    for i, at in enumerate(blocks):
        fetches[i].wait()
        pairs = x_ref[at].astype(F32).reshape(rows // 16, 2, 8, half)
        first, second = swap_halves(pairs[:, 0], pairs[:, 1])
        first = first.reshape(rows // 2, half).astype(BF)
        second = second.reshape(rows // 2, half).astype(BF)
        gate = dot(first, gate_ref[:half]) + dot(second, gate_ref[half:])
        up = dot(first, up_ref[:half]) + dot(second, up_ref[half:])
        hidden = silu_times(gate, up).astype(BF)
        lanes = half // 2
        for j in range(2):
            low = slice(j * lanes, (j + 1) * lanes)
            high = slice(half + j * lanes, half + (j + 1) * lanes)
            first = dot(hidden, down_ref[:, low]).reshape(rows // 16, 8, lanes)
            second = dot(hidden, down_ref[:, high]).reshape(rows // 16, 8, lanes)
            first, second = swap_halves(first, second)
            made_ref[at, low] = jnp.stack([first, second], axis=1).reshape(rows, lanes).astype(BF)
            send = pltpu.make_async_copy(
                made_ref.at[at, low], out_ref.at[at, low], left.at[2 * i + j]
            )
            send.start()
            sends.append(send)
    for send in sends:
        send.wait()


def side_kernel(ids_ref, logits_ref, stats_ref, full_ref, half_ref, loss_ref):
    tok, experts = logits_ref.shape
    devices = stats_ref.shape[0] // 8
    stats = jnp.sum(stats_ref[...].astype(F32).reshape(devices, 8, experts), axis=0)
    total_probs = stats[1:2] + (stats[2:3] + stats[3:4])
    tokens_all = tok * devices
    share = stats[0:1] / (tokens_all * ids_ref.shape[0]) * (total_probs / tokens_all)
    loss_ref[0, 0] = experts * jnp.sum(share)
    hit, slots = slots_by_expert(ids_ref, experts)
    hit = hit.T
    slots = slots.T
    chosen = jnp.where(hit > 0.0, probabilities(logits_ref[...]), 0.0)
    weights = chosen / jnp.sum(chosen, axis=1, keepdims=True)
    columns = experts * 8
    spread = jnp.where(iota((experts, columns), 1) // 8 == iota((experts, columns), 0), 1.0, 0.0).astype(BF)
    wide = dot(slots.astype(BF), spread)
    line = iota(wide.shape, 1) % 8
    in_full = wide == line.astype(F32)
    in_half = wide == (FULL + line % HALF).astype(F32)
    for number, term in enumerate(three_terms(weights)[:2]):
        value = dot(term, spread)
        rows = slice(number * tok, (number + 1) * tok)
        full_ref[rows, :] = jnp.where(in_full, value, 0.0).astype(BF)
        half_ref[rows, :] = jnp.where(in_half & (line < HALF), value, 0.0).astype(BF)
        rows = slice((number + 2) * tok, (number + 3) * tok)
        half_ref[rows, :] = jnp.where(in_half & (line >= HALF), value, 0.0).astype(BF)


def add_terms(product):
    tok = product.shape[0] // 2
    return product[:tok] + product[tok:]


def sum_kernel(full_weights_ref, half_weights_ref, full_ref, hbm_ref, out_ref, half_ref, sofar_ref, made_ref, arrived, left):
    blocks, _, lanes = half_ref.shape
    half = blocks * lanes
    fetches = [
        pltpu.make_async_copy(
            hbm_ref.at[:, i * lanes : (i + 1) * lanes], half_ref.at[i], arrived.at[i]
        )
        for i in range(blocks)
    ]
    for fetch in fetches:
        fetch.start()
    for i in range(2 * blocks):
        at = slice(i * lanes, (i + 1) * lanes)
        sofar_ref[:, at] = add_terms(dot(full_weights_ref[...], full_ref[:, at]))
    sends = []
    for i, fetch in enumerate(fetches):
        fetch.wait()
        rest = dot(half_weights_ref[...], half_ref[i])
        rows = rest.shape[0] // 2
        for side in range(2):
            at = slice(side * half + i * lanes, side * half + (i + 1) * lanes)
            own = add_terms(rest[side * rows : (side + 1) * rows])
            made_ref[:, at] = (sofar_ref[:, at] + own).astype(BF)
            send = pltpu.make_async_copy(
                made_ref.at[:, at], out_ref.at[:, at], left.at[2 * i + side]
            )
            send.start()
            sends.append(send)
    for send in sends:
        send.wait()


def whole(shape):
    zeros = (0,) * len(shape)
    return pl.BlockSpec(shape, lambda *_: zeros, pipeline_mode=pl.Buffered(1))


def call(kernel, grid, out_shape, in_specs, out_specs, flops, moved, limit=20, scratch=()):
    return pl.pallas_call(
        kernel,
        grid=grid,
        out_shape=out_shape,
        in_specs=in_specs,
        out_specs=out_specs,
        scratch_shapes=scratch,
        name=kernel.__name__,
        cost_estimate=pl.CostEstimate(flops=flops, bytes_accessed=moved, transcendentals=0),
        compiler_params=pltpu.CompilerParams(
            dimension_semantics=("arbitrary",) * len(grid), vmem_limit_bytes=limit * 2**20
        ),
    )


def local(tokens, router_logits, expert_ids, w_gate, w_up, w_down):
    tok, top_k = expert_ids.shape
    width = tokens.shape[1]
    experts = router_logits.shape[1]
    ff = w_gate.shape[2]
    devices = lax.axis_size(ROW_COL)
    half = width // 2
    lines = experts * 8
    ids = expert_ids.T
    in_vmem = lambda x: pltpu.with_memory_space_constraint(x, pltpu.VMEM)
    in_hbm = lambda x: pltpu.with_memory_space_constraint(x, pltpu.HBM)
    resident = pl.BlockSpec(memory_space=pltpu.VMEM)
    in_place = pl.BlockSpec(memory_space=pltpu.HBM)
    gate, up, down = in_vmem(w_gate[0]), in_vmem(w_up[0]), in_vmem(w_down[0])
    shape = jax.ShapeDtypeStruct

    def exchange(x):
        lanes = x.shape[1]
        moved = lax.all_to_all(
            x.reshape(experts, 8, lanes), ROW_COL, split_axis=0, concat_axis=0, tiled=True
        )
        return moved.reshape(lines, lanes)

    sent = width + half + experts
    send = call(
        send_kernel,
        (),
        pltpu.VMEM((lines, sent), BF),
        [in_place] * 3,
        resident,
        2 * lines * tok * (width + 2 * half),
        2 * lines * sent,
        scratch=(
            pltpu.VMEM(ids.shape, jnp.int32),
            pltpu.VMEM(router_logits.shape, F32),
            pltpu.VMEM((2 * tok, half), BF),
            pltpu.SemaphoreType.DMA((4,)),
        ),
    )(in_hbm(ids), in_hbm(router_logits), in_hbm(tokens))
    got = in_hbm(exchange(send))
    made_half = call(
        ffn_half_kernel,
        (),
        pltpu.HBM((lines, half), BF),
        [in_place] + [resident] * 3,
        in_place,
        3 * lines * width * ff,
        2 * lines * width + 6 * width * ff,
        34,
        scratch=(
            pltpu.VMEM((lines, half), BF),
            pltpu.VMEM((lines, half), BF),
            pltpu.SemaphoreType.DMA((2,)),
            pltpu.SemaphoreType.DMA((4,)),
        ),
    )(got, gate, up, down)
    back_half = exchange(made_half)
    weights_full, weights_half, loss = call(
        side_kernel,
        (1,),
        (
            shape((2 * tok, lines), BF),
            shape((4 * tok, lines), BF),
            shape((1, 1), F32),
        ),
        [
            whole(ids.shape),
            whole(router_logits.shape),
            pl.BlockSpec((lines, experts), lambda i: (0, (width + half) // experts)),
        ],
        (
            whole((2 * tok, lines)),
            whole((4 * tok, lines)),
            pl.BlockSpec(memory_space=pltpu.SMEM),
        ),
        6 * tok * experts * lines,
        12 * tok * lines,
    )(ids, router_logits, got)
    made_full = call(
        ffn_full_kernel,
        (4,),
        pltpu.HBM((lines, width), BF),
        [
            pl.BlockSpec(memory_space=pl.ANY),
            pl.BlockSpec((lines // 4, width), lambda i: (i, 0)),
        ]
        + [resident] * 3,
        pl.BlockSpec((lines // 4, width), lambda i: (i, 0)),
        6 * lines * width * ff,
        4 * lines * width + 6 * width * ff,
        24,
    )(weights_full, got, gate, up, down)
    back_full = exchange(made_full)

    lanes = half // 4
    mixed = call(
        sum_kernel,
        (),
        pltpu.HBM((tok, width), BF),
        [resident] * 3 + [in_place],
        in_place,
        8 * tok * lines * width,
        2 * lines * (width + half),
        scratch=(
            pltpu.VMEM((4, lines, lanes), BF),
            pltpu.VMEM((tok, width), F32),
            pltpu.VMEM((tok, width), BF),
            pltpu.SemaphoreType.DMA((4,)),
            pltpu.SemaphoreType.DMA((8,)),
        ),
    )(in_vmem(weights_full), in_vmem(weights_half), in_vmem(back_full), in_hbm(back_half))
    return mixed, loss.reshape(())


def solution(mesh):
    torus = Mesh(mesh.devices.reshape(4, 2, 4, 4), ROW_COL)
    rows = P(ROW_COL, None)
    expert = P(ROW_COL, None, None)
    return jax.shard_map(
        local,
        mesh=torus,
        in_specs=(rows, rows, rows, expert, expert, expert),
        out_specs=(rows, P()),
        check_vma=False,
    )
```
